128 devices in a mesh: section: 4 (over y_lo, core), expert: 32 (over x, y_hi, z).
Axes of the slice: x: 4, y: 4 (y_hi: 2, y_lo: 2; y = y_hi * 2 + y_lo), z: 4, core: 2. Of those that a mesh axis runs over, the one named last changes fastest.
Arguments:
- pending_inputs: bfloat16 [4, 1024, 4096], P('section', 'expert'), may hold values from -6 to 6
- arriving_microgroups: bfloat16 [1, 1024, 4096], P(None, 'expert'), may hold values from -6 to 6
- expert_assignment: int32 [4, 2, 1024, 2], P('section', None, 'expert'), may hold values from 0 to 3, all different within a row; in each aligned block of 32 rows (0 to 31, 32 to 63, ..., all dimensions but the last counted through in order) at most 24 rows name the same one
- segment_rescale_factor: float32 [4, 4096], P('section'), may hold values from 0.5 to 1.5
- assignment_logit_maps: float32 [4, 4096, 4], P('section'), may hold values from -0.09375 to 0.09375
- gating_projections: bfloat16 [4, 4096, 28672], P('section', None, 'expert'), may hold values from -0.09375 to 0.09375
- expanding_projections: bfloat16 [4, 4096, 28672], P('section', None, 'expert'), may hold values from -0.09375 to 0.09375
- contracting_projections: bfloat16 [4, 28672, 4096], P('section', 'expert'), may hold values from -0.0625 to 0.0625
Outputs:
- carried: bfloat16 [2, 4, 1024, 4096], P(None, 'section', 'expert')
The draws below stay inside these ranges and needn't reach their ends.
Inputs may be any that keep to these rules, and one draw needn't show every extreme that they name: `expert_assignment`: the two experts of a row differ. Among the rows of one device (one section, one step, 32 tokens), no expert is named more than 24 times, and in every draw some expert is named exactly 24 times.
All inputs are finite; a program needn't handle non-finite values.
Results may differ from the reference program's by a relative error of at most 0.0085.
Values may be sent and summed in bfloat16 or wider, within the bound.
A program may use at most 128 MiB of HBM per device.

```python
import math
import jax
import jax.numpy as jnp
import numpy as np
from jax import lax

HIDDEN_WIDTH = 4096
FF = 7168
EXPERTS = 4
STEPS = 2
TOK_DEV = 32
CAP = 24
MICRO_SEQ_COUNT = 1024
N_SECTION = 4
N_EXPERT = 32


def level_of(rng, dims, cuts, smallest, largest):
    def one(axis_at, shards_of):
        steps = jax.random.uniform(jax.random.fold_in(jax.random.fold_in(rng, 6), axis_at), (shards_of,), jnp.float32, smallest / len(cuts), largest / len(cuts))
        return jnp.repeat(jnp.exp(steps), dims[axis_at] // shards_of).reshape((-1,) + (1,) * (len(dims) - axis_at - 1))

    loudness = one(*cuts[0])
    for cut in cuts[1:]:
        loudness = loudness * one(*cut)
    return loudness


def deal_out(rng, own, number, rows, count, top, most, lean):
    ranking = jax.random.permutation(rng, count)
    crowded, usual = portions_of(count, rows * top, most, lean, True), portions_of(count, rows * top, most, lean, False)
    places = jnp.arange(count)

    def named(sizes, rotation):
        used = int((sizes > 0).sum())
        fixed = max(1, used // 4)
        shifted = fixed + (places - fixed + rotation * (used - fixed)) % max(1, count - fixed)
        return jnp.zeros((count,), jnp.int32).at[ranking[jnp.where(places < fixed, places, shifted)]].set(jnp.asarray(sizes, jnp.int32))

    sizes = jnp.where(number % 4 == 0, named(crowded, number // 4), named(usual, number - number // 4 - 1))
    mixed = jax.random.permutation(jax.random.fold_in(own, 3), count)
    source_of, taker = mixed[0:count // 2 * 2:2], mixed[1:count // 2 * 2:2]
    room = jnp.minimum(sizes[source_of] - 1, most - sizes[taker]) // 2
    room = jnp.where((source_of == ranking[0]) | (taker == ranking[0]) | (sizes[taker] == 0), 0, jnp.maximum(room, 0))
    shifted = jax.random.randint(jax.random.fold_in(own, 4), (count // 2,), 0, 1 << 20) % (room + 1)
    sizes = sizes.at[source_of].add(-shifted).at[taker].add(shifted)
    items = jnp.searchsorted(jnp.cumsum(sizes), jnp.arange(rows * top), side="right").astype(jnp.int32)
    listing = items.reshape(top, rows).T
    listing = listing[jax.random.permutation(jax.random.fold_in(own, 1), rows)]
    rotation = jax.random.randint(jax.random.fold_in(own, 2), (rows, 1), 0, top)
    return jnp.take_along_axis(listing, (jnp.arange(top)[None, :] + rotation) % top, axis=1)


def portions_of(number_of, total, most, skew, full):
    loads = [(1 << 20) // math.isqrt(rank ** skew) + 1 for rank in range(1, number_of + 1)]
    largest = most if full else min(most, max(-(-total // number_of), total * loads[0] // sum(loads)))
    least = 1 if total - largest >= number_of - 1 else 0
    counts, surplus = [largest] + [least] * (number_of - 1), total - largest - least * (number_of - 1)
    while surplus > 0:
        candidates = [i for i in range(1, number_of) if counts[i] < largest] or [i for i in range(1, number_of) if counts[i] < most]
        pool, budget = sum([loads[i] for i in candidates]), surplus
        for i in candidates:
            addition = min(most - counts[i], max(1, budget * loads[i] // pool), surplus)
            counts[i] = counts[i] + addition
            surplus = surplus - addition
    return np.array(counts)


def scatter_about(key, shape, width, bound, pieces=(), kind=jnp.bfloat16):
    entries = width * jax.random.normal(key, shape, jnp.float32)
    if pieces:
        entries = entries * level_of(key, shape, pieces, -0.22, 0.18)
    return jnp.clip(entries, -bound, bound).astype(kind)


def setup_inputs(seed: int = 0) -> dict:
    splits = jax.random.split(jax.random.key(seed), 9)
    pending_inputs = scatter_about(splits[0], (N_SECTION, MICRO_SEQ_COUNT, HIDDEN_WIDTH), 1.0, 6.0, ((0, 4), (1, 32)))
    arriving_microgroups = scatter_about(splits[1], (STEPS - 1, MICRO_SEQ_COUNT, HIDDEN_WIDTH), 1.0, 6.0, ((1, 32),))
    expert_assignment_keys = jax.random.split(jax.random.fold_in(splits[2], 1), N_SECTION * STEPS * MICRO_SEQ_COUNT // TOK_DEV)
    expert_assignment_turns = jax.random.permutation(jax.random.fold_in(splits[2], 3), N_SECTION * STEPS * MICRO_SEQ_COUNT // TOK_DEV)
    expert_assignment = jax.vmap(lambda own, number: deal_out(jax.random.fold_in(splits[2], 2), own, number, TOK_DEV, EXPERTS, 2, CAP, 2))(expert_assignment_keys, expert_assignment_turns).reshape((N_SECTION, STEPS, MICRO_SEQ_COUNT, 2))
    segment_rescale_factor = jnp.clip(0.5 + 1.0 * jax.random.uniform(splits[3], (N_SECTION, HIDDEN_WIDTH), jnp.float32) ** level_of(splits[3], (N_SECTION, HIDDEN_WIDTH), ((0, 4),), -0.2, 0.2), 0.5, 1.5)
    assignment_logit_maps = scatter_about(splits[4], (N_SECTION, HIDDEN_WIDTH, EXPERTS), HIDDEN_WIDTH ** -0.5, 0.09375, ((0, 4),), jnp.float32)
    gating_projections = scatter_about(splits[5], (N_SECTION, HIDDEN_WIDTH, EXPERTS * FF), HIDDEN_WIDTH ** -0.5, 0.09375, ((0, 4), (2, 32)))
    expanding_projections = scatter_about(splits[6], (N_SECTION, HIDDEN_WIDTH, EXPERTS * FF), HIDDEN_WIDTH ** -0.5, 0.09375, ((0, 4), (2, 32)))
    contracting_projections = scatter_about(splits[7], (N_SECTION, EXPERTS * FF, HIDDEN_WIDTH), FF ** -0.5, 0.0625, ((0, 4), (1, 32)))
    return {"pending_inputs": pending_inputs, "arriving_microgroups": arriving_microgroups, "expert_assignment": expert_assignment, "segment_rescale_factor": segment_rescale_factor, "assignment_logit_maps": assignment_logit_maps, "gating_projections": gating_projections, "expanding_projections": expanding_projections, "contracting_projections": contracting_projections}


epsilon = 1e-05

def section_layer(activation, chosen, segment_rescale_factor, assignment_logit_maps, gating_projections, expanding_projections, contracting_projections):
    as_float = activation.astype(jnp.float32)
    normed = (as_float * lax.rsqrt(lax.optimization_barrier(jnp.mean(as_float * as_float, -1, keepdims=True)) + epsilon) * segment_rescale_factor).astype(jnp.bfloat16)
    logits = jnp.dot(normed.astype(jnp.float32), assignment_logit_maps, precision=lax.Precision.HIGHEST)
    chooses = chosen[:, :, None] == jnp.arange(EXPERTS, dtype=jnp.int32)[None, None, :]
    picked = lax.optimization_barrier(jnp.sum(jnp.where(chooses, logits[:, None, :], jnp.float32(0.0)), -1))
    first_share = jax.nn.sigmoid(picked[:, 0] - picked[:, 1])
    shares = jnp.stack([first_share, 1.0 - first_share], 1).astype(jnp.bfloat16).astype(jnp.float32).reshape(-1)
    chosen_flat = chosen.reshape(-1).astype(jnp.int32)
    token_owner = (jnp.arange(2 * MICRO_SEQ_COUNT, dtype=jnp.int32) // 2).astype(jnp.int32)
    capacity = N_EXPERT * CAP

    def one_expert(expert_id):
        matches = chosen_flat == expert_id
        index_list = jnp.nonzero(matches, size=capacity, fill_value=0)[0].astype(jnp.int32)
        live = jnp.arange(capacity, dtype=jnp.int32) < jnp.sum(matches.astype(jnp.int32))
        owners = token_owner[index_list]
        token_rows = normed[owners]
        gate_cols = lax.dynamic_slice_in_dim(gating_projections, (expert_id * FF).astype(jnp.int32), FF, 1)
        up_cols = lax.dynamic_slice_in_dim(expanding_projections, (expert_id * FF).astype(jnp.int32), FF, 1)
        down_rows = lax.dynamic_slice_in_dim(contracting_projections, (expert_id * FF).astype(jnp.int32), FF, 0)
        gate_value = jnp.dot(token_rows, gate_cols, preferred_element_type=jnp.float32)
        up_value = jnp.dot(token_rows, up_cols, preferred_element_type=jnp.float32)
        hidden = (jax.nn.silu(gate_value) * up_value).astype(jnp.bfloat16)
        output = jnp.dot(hidden, down_rows, preferred_element_type=jnp.float32)
        weight = jnp.where(live, shares[index_list], jnp.float32(0.0))
        return jnp.zeros((MICRO_SEQ_COUNT, HIDDEN_WIDTH), jnp.float32).at[owners].add(output * weight[:, None])
    mixture = lax.optimization_barrier(jnp.sum(lax.map(one_expert, jnp.arange(EXPERTS, dtype=jnp.int32)), 0))
    return (as_float + mixture).astype(jnp.bfloat16)

def reference(pending_inputs, arriving_microgroups, expert_assignment, segment_rescale_factor, assignment_logit_maps, gating_projections, expanding_projections, contracting_projections):
    activation_sequence = [pending_inputs[segment_ordinal] for segment_ordinal in range(N_SECTION)]
    records = []
    for step_index in range(STEPS):
        if step_index > 0:
            activation_sequence[0] = arriving_microgroups[step_index - 1]
        results = [section_layer(activation_sequence[segment_ordinal], expert_assignment[segment_ordinal, step_index], segment_rescale_factor[segment_ordinal], assignment_logit_maps[segment_ordinal], gating_projections[segment_ordinal], expanding_projections[segment_ordinal], contracting_projections[segment_ordinal]) for segment_ordinal in range(N_SECTION)]
        activation_sequence = [results[(segment_ordinal - 1) % N_SECTION] for segment_ordinal in range(N_SECTION)]
        records.append(jnp.stack(activation_sequence))
    return jnp.stack(records)
```

```python
import jax
import jax.numpy as jnp
from jax import lax
from jax.sharding import PartitionSpec as P

EXPERTS = 4
STEPS = 2

epsilon = 1e-05


def shifted(x, axis, by):
    size = lax.axis_size(axis)
    return lax.ppermute(x, axis, [(i, (i + by) % size) for i in range(size)])


def moe_layer(activation, chosen, gain, router, gate_cols, up_cols, down_rows, group_size):
    as_float = activation.astype(jnp.float32)
    normed = (
        as_float
        * lax.rsqrt(jnp.mean(as_float * as_float, -1, keepdims=True) + epsilon)
        * gain
    ).astype(jnp.bfloat16)
    logits = jnp.dot(normed.astype(jnp.float32), router, precision=lax.Precision.HIGHEST)
    chooses = chosen[:, :, None] == jnp.arange(EXPERTS, dtype=jnp.int32)[None, None, :]
    picked = jnp.sum(jnp.where(chooses, logits[:, None, :], 0.0), -1)
    first_share = jax.nn.sigmoid(picked[:, 0] - picked[:, 1])
    share_pair = jnp.stack([first_share, 1.0 - first_share], 1).astype(jnp.bfloat16)
    weights = jnp.sum(jnp.where(chooses, share_pair[:, :, None].astype(jnp.float32), 0.0), 1)
    width = activation.shape[-1]
    extra = jnp.pad(weights.astype(jnp.bfloat16), ((0, 0), (0, 128 - EXPERTS)))
    packed = jnp.concatenate([normed, extra], 1)
    every = lax.all_gather(packed, "expert", axis=0, tiled=True)
    rows = every[:, :width]
    mine = lax.axis_index("expert") // group_size
    lanes = jnp.arange(128, dtype=jnp.int32)[None, :] == mine
    weight = jnp.sum(jnp.where(lanes, every[:, width:].astype(jnp.float32), 0.0), 1)
    gate_value = jnp.dot(rows, gate_cols, preferred_element_type=jnp.float32)
    up_value = jnp.dot(rows, up_cols, preferred_element_type=jnp.float32)
    hidden = (jax.nn.silu(gate_value) * up_value).astype(jnp.bfloat16)
    output = jnp.dot(hidden, down_rows, preferred_element_type=jnp.float32) * weight[:, None]
    mixture = lax.psum_scatter(
        output.astype(jnp.bfloat16), "expert", scatter_dimension=0, tiled=True
    )
    return (as_float + mixture.astype(jnp.float32)).astype(jnp.bfloat16)


def shards(
    pending_inputs,
    arriving_microgroups,
    expert_assignment,
    segment_rescale_factor,
    assignment_logit_maps,
    gating_projections,
    expanding_projections,
    contracting_projections,
):
    section_index = lax.axis_index("section")
    group_size = lax.axis_size("expert") // EXPERTS
    present_activation = pending_inputs[0]
    records = []
    for step_index in range(STEPS):
        if step_index > 0:
            present_activation = jnp.where(
                section_index == 0, arriving_microgroups[step_index - 1], present_activation
            )
        result = moe_layer(
            present_activation,
            expert_assignment[0, step_index],
            segment_rescale_factor[0],
            assignment_logit_maps[0],
            gating_projections[0],
            expanding_projections[0],
            contracting_projections[0],
            group_size,
        )
        present_activation = shifted(result, "section", 1)
        records.append(present_activation)
    return jnp.stack(records)[:, None]


def solution(mesh):
    return jax.shard_map(
        shards,
        mesh=mesh,
        in_specs=(
            P("section", "expert", None),
            P(None, "expert", None),
            P("section", None, "expert", None),
            P("section", None),
            P("section", None, None),
            P("section", None, "expert"),
            P("section", None, "expert"),
            P("section", "expert", None),
        ),
        out_specs=P(None, "section", "expert", None),
        check_vma=False,
    )
```

```python
import jax
import jax.numpy as jnp
from jax import lax
from jax.experimental import pallas as pl
from jax.experimental.pallas import tpu as pltpu
from jax.sharding import PartitionSpec as P

EXPERTS = 4
STEPS = 2
EXTRA = 128
BLOCK = 16
LANE = 128

epsilon = 1e-05

OWN, PLUS, MINUS, FAR = 0, 1, 2, 3
SLAB = (
    {OWN: 0, PLUS: 2, MINUS: 3, FAR: 6},
    {OWN: 1, PLUS: 4, MINUS: 5, FAR: 7},
)


def row_of(color, last, half, middle):
    return SLAB[color][last] * 128 + half * 64 + middle * 16


def shifted(x, axis, by):
    size = lax.axis_size(axis)
    return lax.ppermute(x, axis, [(i, (i + by) % size) for i in range(size)])


BUNDLES = ((0, OWN), (0, MINUS), (0, PLUS), (1, OWN), (0, FAR), (1, MINUS), (1, PLUS), (1, FAR))


def step_kernel(
    packed_ref, x_ref, gate_hbm, up_hbm, down_hbm, out_ref,
    rows, wide, down, hidden, part, ring_last, ring_mid, y_in, share,
    send_sems, recv_sems, load_sems,
):
    width = x_ref.shape[1]
    half_w = width // 2
    full = packed_ref.shape[1]
    ff = down.shape[0]
    tiles = ff // LANE
    section = lax.axis_index("section")
    e = lax.axis_index("expert")
    cx, cy, cz = e // 8, (e // 4) % 2, e % 4

    def at(x, y, z):
        return {"section": section, "expert": x * 8 + y * 4 + z}

    x_up = at(lax.rem(cx + 1, 4), cy, cz)
    x_dn = at(lax.rem(cx + 3, 4), cy, cz)
    z_up = at(cx, cy, lax.rem(cz + 1, 4))
    z_dn = at(cx, cy, lax.rem(cz + 3, 4))
    partner = at(cx, 1 - cy, cz)
    mid_to = ((x_up, x_dn), (z_up, z_dn))
    last_to = ((z_up, z_dn), (x_up, x_dn))

    loads = []

    def load(src, dst):
        copy = pltpu.make_async_copy(src, dst, load_sems.at[len(loads)])
        copy.start()
        loads.append(copy)

    for j in range(tiles):
        load(gate_hbm.at[:, pl.ds(j * LANE, LANE)], wide.at[j, :, pl.ds(0, LANE)])
        load(up_hbm.at[:, pl.ds(j * LANE, LANE)], wide.at[j, :, pl.ds(LANE, LANE)])
    load(down_hbm, down)

    barrier = pltpu.get_barrier_semaphore()
    for device in (x_up, x_dn, z_up, z_dn, partner):
        pl.semaphore_signal(barrier, inc=1, device_id=device, device_id_type=pl.DeviceIdType.MESH)
    pl.semaphore_wait(barrier, 5)

    sent = []
    coming = {}

    def send(key, src, dst, device):
        n = len(sent)
        copy = pltpu.make_async_remote_copy(
            src_ref=src, dst_ref=dst, send_sem=send_sems.at[n], recv_sem=recv_sems.at[n],
            device_id=device, device_id_type=pl.DeviceIdType.MESH,
        )
        copy.start()
        sent.append(copy)
        coming[key] = copy

    def arrive(key):
        coming[key].wait_recv()

    left = (pl.ds(0, half_w), pl.ds(half_w, full - half_w))

    def block(color, last, half, middle):
        return pl.ds(row_of(color, last, half, middle), BLOCK)

    def along_mid(c, half):
        for way, slot in ((0, MINUS), (1, PLUS)):
            src = (
                packed_ref.at[pl.ds(c * BLOCK, BLOCK)]
                if half == 0
                else rows.at[block(c, OWN, 1, OWN)]
            )
            send(("mid", c, half, way), src, rows.at[block(c, OWN, half, slot)], mid_to[c][way])

    def forward_mid(c, half, way):
        slot = (MINUS, PLUS)[way]
        send(
            ("midfar", c, half, way),
            rows.at[block(c, OWN, half, slot), left[way]],
            rows.at[block(c, OWN, half, FAR), left[way]],
            mid_to[c][way],
        )

    def along_last(c, k):
        half, middle = BUNDLES[k]
        src = (
            packed_ref.at[pl.ds(c * BLOCK, BLOCK)]
            if k == 0
            else rows.at[block(c, OWN, half, middle)]
        )
        for way, slot in ((0, MINUS), (1, PLUS)):
            send(("last", c, k, way), src, rows.at[block(c, slot, half, middle)], last_to[c][way])

    def forward_last(c, k, way):
        half, middle = BUNDLES[k]
        slot = (MINUS, PLUS)[way]
        send(
            ("lastfar", c, k, way),
            rows.at[block(c, slot, half, middle), left[way]],
            rows.at[block(c, FAR, half, middle), left[way]],
            last_to[c][way],
        )

    for c in (0, 1):
        along_mid(c, 0)
        send(
            ("y", c), packed_ref.at[pl.ds(c * BLOCK, BLOCK)], rows.at[block(c, OWN, 1, OWN)], partner
        )
    for c in (0, 1):
        along_last(c, 0)
    for c in (0, 1):
        rows[block(c, OWN, 0, OWN), :] = packed_ref[pl.ds(c * BLOCK, BLOCK), :]

    def pass_last(k):
        for c in (0, 1):
            for way in (0, 1):
                arrive(("last", c, k, way))
                forward_last(c, k, way)

    for way, k in ((0, 1), (1, 2)):
        for c in (0, 1):
            arrive(("mid", c, 0, way))
            forward_mid(c, 0, way)
            along_last(c, k)
    for c in (0, 1):
        arrive(("y", c))
        along_mid(c, 1)
        along_last(c, 3)
    pass_last(0)
    for c in (0, 1):
        for way in (0, 1):
            arrive(("midfar", c, 0, way))
        along_last(c, 4)
    pass_last(1)
    for way, k in ((0, 5), (1, 6)):
        for c in (0, 1):
            arrive(("mid", c, 1, way))
            forward_mid(c, 1, way)
            along_last(c, k)
    pass_last(2)
    for c in (0, 1):
        for way in (0, 1):
            arrive(("midfar", c, 1, way))
        along_last(c, 7)

    def make_hidden(s):
        @pl.loop(0, tiles)
        def _(j):
            both = jnp.dot(
                rows[pl.ds(s * 256, 256), pl.ds(0, width)], wide[j],
                preferred_element_type=jnp.float32,
            )
            gate = both[:, :LANE]
            value = gate / (1.0 + jnp.exp(-gate)) * both[:, LANE:]
            hidden[pl.ds(s * 256, 256), pl.ds(pl.multiple_of(j * LANE, LANE), LANE)] = value.astype(
                jnp.bfloat16
            )

    lanes = lax.broadcasted_iota(jnp.int32, (256, EXTRA), 1)

    def make_part(s):
        tags = rows[pl.ds(s * 256, 256), pl.ds(width, EXTRA)].astype(jnp.float32)
        share[...] = jnp.sum(jnp.where(lanes == cx, tags, 0.0), 1, keepdims=True)

        @pl.loop(0, width // 512)
        def _(j):
            cols = pl.ds(pl.multiple_of(j * 512, 512), 512)
            value = jnp.dot(
                hidden[pl.ds(s * 256, 256), :], down[:, cols], preferred_element_type=jnp.float32
            )
            part[pl.ds(s * 256, 256), cols] = (value * share[...]).astype(jnp.bfloat16)

    for copy in loads[:-1]:
        copy.wait()
    make_hidden(0)
    loads[-1].wait()
    for k in range(3, 8):
        pass_last(k)

    sides = (pl.ds(0, half_w), pl.ds(half_w, half_w))

    def reduce_send(stage, c, half, way, kind):
        near = (PLUS, MINUS)[way]
        target = FAR if kind == 1 else near
        side = sides[1 - way] if kind == 0 else sides[way]
        if stage == "last":
            src = part.at[pl.ds(row_of(c, target, half, OWN), 64), side]
            dst = ring_last.at[c, half, way, kind]
            device = last_to[c][way]
        else:
            src = part.at[block(c, OWN, half, target), side]
            dst = ring_mid.at[c, half, way, kind]
            device = mid_to[c][way]
        send((stage, c, half, way, kind, "r"), src, dst, device)

    def reduce_pass(stage, c, half, way):
        arrive((stage, c, half, way, 1, "r"))
        near = (PLUS, MINUS)[way]
        side = sides[way]
        count = 4 if stage == "last" else 1
        base = row_of(c, near, half, OWN) if stage == "last" else row_of(c, OWN, half, near)
        landed = (ring_last if stage == "last" else ring_mid).at[c, half, way, 1]

        @pl.loop(0, count)
        def _(i):
            off = pl.multiple_of(i * BLOCK, BLOCK)
            here = pl.ds(pl.multiple_of(base + off, BLOCK), BLOCK)
            total = part[here, side].astype(jnp.float32) + landed[pl.ds(off, BLOCK), :].astype(
                jnp.float32
            )
            part[here, side] = total.astype(jnp.bfloat16)

        reduce_send(stage, c, half, way, 2)

    def reduce_end(stage, c, half):
        for way in (0, 1):
            arrive((stage, c, half, way, 0, "r"))
            arrive((stage, c, half, way, 2, "r"))
        count = 4 if stage == "last" else 1
        base = row_of(c, OWN, half, OWN)
        landed = (ring_last if stage == "last" else ring_mid).at[c, half]

        @pl.loop(0, count)
        def _(i):
            off = pl.multiple_of(i * BLOCK, BLOCK)
            here = pl.ds(pl.multiple_of(base + off, BLOCK), BLOCK)
            for way in (0, 1):
                total = (
                    part[here, sides[way]].astype(jnp.float32)
                    + landed[1 - way, 0, pl.ds(off, BLOCK), :].astype(jnp.float32)
                    + landed[way, 2, pl.ds(off, BLOCK), :].astype(jnp.float32)
                )
                part[here, sides[way]] = total.astype(jnp.bfloat16)

    make_hidden(1)
    make_part(1)
    for half in (1, 0):
        for way in (0, 1):
            reduce_send("last", 0, half, way, 0)
    make_hidden(2)
    make_part(2)
    for half in (1, 0):
        for way in (0, 1):
            reduce_send("last", 1, half, way, 0)
    for k in range(8):
        for c in (0, 1):
            for way in (0, 1):
                arrive(("lastfar", c, k, way))
    make_hidden(3)
    make_part(3)
    for half in (1, 0):
        for c in (0, 1):
            for way in (0, 1):
                reduce_send("last", c, half, way, 1)
    make_part(0)
    for half in (1, 0):
        for c in (0, 1):
            for way in (0, 1):
                reduce_pass("last", c, half, way)
    for half in (1, 0):
        for c in (0, 1):
            reduce_end("last", c, half)
            for way in (0, 1):
                reduce_send("mid", c, half, way, 1)
            for way in (0, 1):
                reduce_send("mid", c, half, way, 0)
    for half in (1, 0):
        for c in (0, 1):
            for way in (0, 1):
                reduce_pass("mid", c, half, way)
    for c in (0, 1):
        reduce_end("mid", c, 1)
        send(("ysum", c), part.at[block(c, OWN, 1, OWN)], y_in.at[c], partner)
    for c in (0, 1):
        reduce_end("mid", c, 0)
    for c in (0, 1):
        arrive(("ysum", c))
        here = pl.ds(c * BLOCK, BLOCK)
        total = (
            x_ref[here, :].astype(jnp.float32)
            + part[block(c, OWN, 0, OWN), :].astype(jnp.float32)
            + y_in[c].astype(jnp.float32)
        )
        out_ref[here, :] = total.astype(jnp.bfloat16)
    for copy in sent:
        copy.wait_send()


def copies_count():
    gather = 2 * (1 + 2 * 4 + 8 * 4)
    reduce = 2 * (2 * 2 * 3 + 2 * 2 * 3 + 1)
    return gather + reduce


def expert_step(packed, activation, gate_cols, up_cols, down_rows):
    tokens, width = activation.shape
    ff = gate_cols.shape[1]
    bf16 = jnp.bfloat16
    total = 1024
    return pl.pallas_call(
        step_kernel,
        out_shape=jax.ShapeDtypeStruct((tokens, width), bf16),
        in_specs=[pl.BlockSpec(memory_space=pltpu.VMEM)] * 2
        + [pl.BlockSpec(memory_space=pl.ANY)] * 3,
        out_specs=pl.BlockSpec(memory_space=pltpu.VMEM),
        scratch_shapes=[
            pltpu.VMEM((total, width + EXTRA), bf16),
            pltpu.VMEM((ff // LANE, width, 2 * LANE), bf16),
            pltpu.VMEM((ff, width), bf16),
            pltpu.VMEM((total, ff), bf16),
            pltpu.VMEM((total, width), bf16),
            pltpu.VMEM((2, 2, 2, 3, 64, width // 2), bf16),
            pltpu.VMEM((2, 2, 2, 3, BLOCK, width // 2), bf16),
            pltpu.VMEM((2, BLOCK, width), bf16),
            pltpu.VMEM((256, 1), jnp.float32),
            pltpu.SemaphoreType.DMA((copies_count(),)),
            pltpu.SemaphoreType.DMA((copies_count(),)),
            pltpu.SemaphoreType.DMA((2 * (ff // LANE) + 1,)),
        ],
        compiler_params=pltpu.CompilerParams(
            collective_id=0, has_side_effects=True, vmem_limit_bytes=64_000_000
        ),
        name="expert_step",
    )(packed, activation, gate_cols, up_cols, down_rows)


def moe_layer(activation, chosen, gain, router, gate_cols, up_cols, down_rows):
    as_float = activation.astype(jnp.float32)
    normed = (
        as_float
        * lax.rsqrt(jnp.mean(as_float * as_float, -1, keepdims=True) + epsilon)
        * gain
    ).astype(jnp.bfloat16)
    logits = jnp.dot(normed.astype(jnp.float32), router, precision=lax.Precision.HIGHEST)
    chooses = chosen[:, :, None] == jnp.arange(EXPERTS, dtype=jnp.int32)[None, None, :]
    picked = jnp.sum(jnp.where(chooses, logits[:, None, :], 0.0), -1)
    first_share = jax.nn.sigmoid(picked[:, 0] - picked[:, 1])
    share_pair = jnp.stack([first_share, 1.0 - first_share], 1).astype(jnp.bfloat16)
    weights = jnp.sum(jnp.where(chooses, share_pair[:, :, None].astype(jnp.float32), 0.0), 1)
    extra = jnp.pad(weights.astype(jnp.bfloat16), ((0, 0), (0, EXTRA - EXPERTS)))
    packed = jnp.concatenate([normed, extra], 1)
    return expert_step(packed, activation, gate_cols, up_cols, down_rows)


def shards(
    pending_inputs,
    arriving_microgroups,
    expert_assignment,
    segment_rescale_factor,
    assignment_logit_maps,
    gating_projections,
    expanding_projections,
    contracting_projections,
):
    section_index = lax.axis_index("section")
    present_activation = pending_inputs[0]
    records = []
    for step_index in range(STEPS):
        if step_index > 0:
            present_activation = jnp.where(
                section_index == 0, arriving_microgroups[step_index - 1], present_activation
            )
        result = moe_layer(
            present_activation,
            expert_assignment[0, step_index],
            segment_rescale_factor[0],
            assignment_logit_maps[0],
            gating_projections[0],
            expanding_projections[0],
            contracting_projections[0],
        )
        present_activation = shifted(result, "section", 1)
        records.append(present_activation)
    return jnp.stack(records)[:, None]


def solution(mesh):
    return jax.shard_map(
        shards,
        mesh=mesh,
        in_specs=(
            P("section", "expert", None),
            P(None, "expert", None),
            P("section", None, "expert", None),
            P("section", None),
            P("section", None, None),
            P("section", None, "expert"),
            P("section", None, "expert"),
            P("section", "expert", None),
        ),
        out_specs=P(None, "section", "expert", None),
        check_vma=False,
    )
```

```python
import jax
import jax.numpy as jnp
from jax import lax
from jax.experimental import pallas as pl
from jax.experimental.pallas import tpu as pltpu
from jax.sharding import PartitionSpec as P

EXPERTS = 4
STEPS = 2
EXTRA = 128
BLOCK = 16
LANE = 128
MESH = pl.DeviceIdType.MESH

epsilon = 1e-05

OWN, PLUS, MINUS, FAR = 0, 1, 2, 3
CAME = (MINUS, PLUS)
GOES = (PLUS, MINUS)
ALL = slice(None)

COLS = {"A": (0, 1024), "B": (1024, 1792), "C": (2816, 1280)}
TILE = 512

SCHEDULE = (
    (0, 1, 3, 5, 23, 25, 27, 45, 47, 151, 152, 154, 156, 174, 176, 178, 196, 198, 4, 6, 26, 28, 46, 48, 2,
     13, 15, 155, 157, 24, 35, 37, 177, 179, 197, 199, 153, 164, 166, 7, 8, 10, 29, 30, 32, 49, 50, 52, 55,
     14, 175, 16, 158, 200, 36, 38, 180, 206, 165, 167, 181, 183, 9, 11, 31, 33, 17, 18, 20, 168, 51, 53,
     56, 57, 39, 40, 42, 12, 169, 171, 19, 21, 34, 54, 58, 186, 182, 184, 188, 201, 203, 41, 43, 22, 170,
     172, 185, 187, 189, 159, 161, 44, 59,),
    (),
    (173, 190, 191, 193, 202, 204, 207,),
    (),
    (160, 162,),
    (208,),
    (205,),
    (163,),
    (192, 194, 209,),
    (60, 61, 64, 65, 77, 78, 81, 82,),
    (),
    (),
    (195, 62, 66,),
    (110, 114, 93, 94, 97, 98,),
    (),
    (79, 83, 128, 210, 132, 111, 115,),
    (126,),
    (112, 116, 63, 67,),
    (68, 69, 72, 73, 80, 84, 95, 99, 130,),
    (),
    (129, 135, 86, 90, 85, 89,),
    (),
    (133, 134, 138,),
    (),
    (70, 74, 113, 117, 118, 119, 122, 123, 211, 212, 215, 216,),
    (127, 136, 232,),
    (87, 91, 96, 71, 75, 76, 100, 101, 102, 105, 106, 120, 124,),
    (131, 139, 140, 228,),
    (261, 265, 88, 92, 229, 244, 248,),
    (),
    (107, 103, 234, 279, 245, 249, 213, 283, 125, 121, 233, 262, 266, 230, 137, 147, 142, 217, 277, 141,
     143, 146, 104, 108, 109, 263, 267, 214, 235, 280, 286, 219, 224, 231, 246, 250, 281, 218, 144, 148,
     284, 285, 289, 220, 223, 237, 241, 236, 240, 264, 268, 269, 270, 273, 221, 274, 278, 287, 247, 251,
     252, 253, 256, 257, 271, 145, 149, 150, 275, 225, 238, 242, 222, 258, 282, 254, 226, 227, 290, 291,
     239, 243, 276, 272, 302, 303, 305, 307, 325, 327, 329, 347, 349, 255, 259, 260, 288, 298, 293, 306,
     308, 292, 294, 297, 328, 348, 350, 304, 315, 317, 330, 295, 326, 337, 309, 339, 310, 312, 299, 351,
     352, 354, 357, 331, 332, 334, 316, 318, 296, 300, 301, 338, 340, 311, 313, 453, 454, 333, 335, 456,
     458, 476, 319, 320, 322, 498, 500, 478, 480, 353, 358, 355, 359, 341, 342, 344, 314, 455, 336, 477,
     488, 490, 321, 457, 323, 459, 466, 468, 499, 501, 479, 481, 356, 360, 489, 491, 343, 345, 460, 461,
     463, 324, 467, 469, 482, 483, 485, 502, 503, 505, 508, 492, 346, 493, 495, 470, 471, 473, 361,),
    (462, 464,),
    (),
    (504, 506, 509, 484, 486,),
    (510,),
    (472, 474,),
    (465,),
    (494, 496,),
    (507, 511,),
    (475, 487, 362, 366,),
    (363, 367,),
    (497,),
    (379, 383,),
    (412, 416, 380, 384,),
    (),
    (430, 395, 381, 385, 512, 399,),
    (364, 368,),
    (434, 414, 418,),
    (382, 386,),
    (365, 369, 370, 371, 374, 375,),
    (396, 400, 428, 431, 437,),
    (),
    (372, 376, 397, 401, 432, 435, 436, 440,),
    (),
    (373, 377, 413, 417, 513, 514, 517, 518, 530, 534,),
    (378, 429, 531, 535,),
    (398, 402, 388, 392, 387, 391,),
    (515, 519,),
    (563, 567, 415, 419, 433, 546, 550,),
    (532, 536, 547, 551,),
    (581, 403, 407, 585, 404, 408, 564, 568, 516, 520, 420, 424, 421, 425, 438, 441, 533, 537, 565, 569,
     579, 405, 409, 422, 426, 442, 521, 525, 522, 526, 548, 552, 583, 439, 582, 588, 406, 410, 423, 427,
     539, 543, 538, 542, 443, 586, 587, 591, 566, 570, 571, 572, 575, 523, 527, 576, 445, 449, 389, 393,
     411, 580, 444, 448, 589, 549, 553, 554, 555, 558, 559, 573, 577, 540, 544, 524, 528, 529, 390, 394,
     446, 450, 584, 592, 593, 560, 541, 545, 556, 578, 447, 451, 452, 574, 590, 600, 595, 557, 594, 596,
     599, 561, 562, 597, 601, 598, 602, 603,),
)


def kernel(
    pending_ref, arriving_ref, chosen_ref, gain_ref, router_ref, gate_hbm, up_hbm, down_hbm, out_ref,
    rows, part, wide, down, hidden, share, mine, relay,
    land_last, land_mid, land_y,
    send_sems, recv_sems, load_sems,
):
    width = pending_ref.shape[1]
    tiles = down.shape[0] // LANE
    section = lax.axis_index("section")
    e = lax.axis_index("expert")
    cx, cy, cz = e // 8, (e // 4) % 2, e % 4

    def at(x, y, z):
        return {"section": section, "expert": x * 8 + y * 4 + z}

    to_x = (at(lax.rem(cx + 1, 4), cy, cz), at(lax.rem(cx + 3, 4), cy, cz))
    to_z = (at(cx, cy, lax.rem(cz + 1, 4)), at(cx, cy, lax.rem(cz + 3, 4)))
    partner = at(cx, 1 - cy, cz)
    following = {"section": lax.rem(section + 1, 4), "expert": e}
    preceding = {"section": lax.rem(section + 3, 4), "expert": e}

    loads = []

    def load(src, dst):
        copy = pltpu.make_async_copy(src, dst, load_sems.at[len(loads)])
        copy.start()
        loads.append(copy)

    for j in range(tiles):
        load(gate_hbm.at[:, pl.ds(j * LANE, LANE)], wide.at[j, :, pl.ds(0, LANE)])
        load(up_hbm.at[:, pl.ds(j * LANE, LANE)], wide.at[j, :, pl.ds(LANE, LANE)])
    load(down_hbm, down)

    barrier = pltpu.get_barrier_semaphore()
    for device in (*to_x, *to_z, partner, following, preceding):
        pl.semaphore_signal(barrier, inc=1, device_id=device, device_id_type=MESH)

    numbers = {}
    known = {}
    flying = {}

    def send(key, group, src, dst, device):
        n = numbers.setdefault(key if "relay" in key else key[1:], len(numbers))
        known[key] = lambda: pltpu.make_async_remote_copy(
            src_ref=src(), dst_ref=dst(), send_sem=send_sems.at[n], recv_sem=recv_sems.at[n],
            device_id=device, device_id_type=MESH,
        )
        known[key]().start()
        flying.setdefault(group, []).append(known[key])

    def arrive(key):
        known[key]().wait_recv()

    def drain(group):
        for copy in flying.pop(group, []):
            copy().wait_send()

    def gathered(h, z, y, x, cols):
        return lambda: rows.at[h, z, y, x, :, cols]

    def summed(h, z, y, x, cols):
        return lambda: part.at[h, z, y, x, :, cols]

    def span(color, tags=False):
        start, size = COLS[color]
        if tags and color == "C":
            size += EXTRA
        cut = size // 2 // LANE * LANE
        return pl.ds(start, size), (pl.ds(start, cut), pl.ds(start + cut, size - cut))

    def source(s, h):
        here = pl.ds(h * BLOCK, BLOCK)
        if s == 0:
            return pending_ref[here, :].astype(jnp.float32)
        return jnp.where(section == 0, arriving_ref[here, :], relay[0, here, :]).astype(jnp.float32)

    def enter(s, h):
        here = pl.ds(h * BLOCK, BLOCK)
        value = source(s, h)
        mean = jnp.mean(value * value, -1, keepdims=True)
        normed = (value * lax.rsqrt(mean + epsilon) * gain_ref[...]).astype(jnp.bfloat16)
        rows[h, 0, 0, 0, :, pl.ds(0, width)] = normed
        precise = normed.astype(jnp.float32)
        lane = lax.broadcasted_iota(jnp.int32, (BLOCK, EXTRA), 1)
        first_choice = chosen_ref[s, here, 0:1]
        second_choice = chosen_ref[s, here, 1:2]
        gap = jnp.zeros((BLOCK, 1), jnp.float32)
        for expert in range(EXPERTS):
            logit = jnp.sum(precise * router_ref[expert : expert + 1, :], -1, keepdims=True)
            gap = gap + jnp.where(first_choice == expert, logit, 0.0)
            gap = gap - jnp.where(second_choice == expert, logit, 0.0)
        first = 1.0 / (1.0 + jnp.exp(-gap))
        second = 1.0 - first
        tags = jnp.where(lane == first_choice, first, 0.0) + jnp.where(
            lane == second_choice, second, 0.0
        )
        rows[h, 0, 0, 0, :, pl.ds(width, EXTRA)] = tags.astype(jnp.bfloat16)

    events = {}

    def event(s, h, label, keys, needs, act):
        def run():
            for key in keys:
                arrive(key)
            act()

        events[s, h, label] = Event(keys, needs, run)

    def gather(s, h):
        group = ("g", s, h)

        def key(tag, way=0):
            return (s, h, "g", tag, way)

        def near(tag, color, to, place, way):
            cols = span(color, True)[0]
            send(key(tag, way), group, gathered(h, *place(OWN), cols),
                 gathered(h, *place(CAME[way]), cols), to[way])

        def ring(tag, color, to, place, needs):
            sides = span(color, True)[1]
            for way in (0, 1):
                event(s, h, (tag, "n", way), [], needs,
                      lambda way=way: near(tag, color, to, place, way))

                def forward(way=way):
                    send(key(tag + "f", way), group, gathered(h, *place(CAME[way]), sides[way]),
                         gathered(h, *place(FAR), sides[way]), to[way])

                event(s, h, (tag, "f", way), [key(tag, way)], [(tag, "n", way)], forward)
            event(s, h, (tag, "e", 0), [key(tag + "f", 0), key(tag + "f", 1)],
                  [(tag, "f", 0), (tag, "f", 1)], lambda: None)
            return (tag, "e", 0)

        def across(tag, color, z, x, needs):
            cols = span(color, True)[0]
            event(s, h, (tag, "n", 0), [], needs, lambda: send(
                key(tag), group, gathered(h, z, 0, x, cols), gathered(h, z, 1, x, cols), partner))
            return key(tag)

        ready = ("enter", "e", 0)
        before = [(s - 1, h, "r", "relay", 0)] if s else []
        event(s, h, ready, before, [("sum", "e", 0)] if s else [], lambda: enter(s, h))
        finals, ends = [], []
        for color in "AB":
            to_mid, to_last = (to_x, to_z) if color == "A" else (to_z, to_x)
            crossed = across(color + "y", color, OWN, OWN, [ready])
            event(s, h, (color + "y", "e", 0), [crossed], [(color + "y", "n", 0)], lambda: None)
            for y in (0, 1):
                mid = (lambda p, y=y: (OWN, y, p)) if color == "A" else (lambda p, y=y: (p, y, OWN))
                last = (lambda p, y=y: (p, y, ALL)) if color == "A" else (lambda p, y=y: (ALL, y, p))
                end = ring(f"{color}m{y}", color, to_mid, mid, [(color + "y", "e", 0) if y else ready])
                ends.append(ring(f"{color}l{y}", color, to_last, last, [end]))
        end_x = ring("Cx", "C", to_x, lambda p: (OWN, 0, p), [ready])
        end_z = ring("Cz", "C", to_z, lambda p: (p, 0, ALL), [end_x])
        for place, need in ((OWN, end_x), (MINUS, ("Cz", "f", 0)), (PLUS, ("Cz", "f", 1)), (FAR, end_z)):
            finals.append(across(f"Cy{place}", "C", place, ALL, [need]))
        event(s, h, ("gathered", "e", 0), finals, ends + [end_z] + [(f"Cy{p}", "n", 0) for p in range(4)],
              lambda: None)

    def reduce(s, h):
        group = ("r", s, h)

        def key(tag, way=0, kind=0):
            return (s, h, "r", tag, way, kind)

        def ring(tag, color, to, place, landing, needs):
            sides = span(color)[1]

            def go(way, kind):
                target = FAR if kind == 1 else GOES[way]
                side = sides[1 - way] if kind == 0 else sides[way]
                send(key(tag, way, kind), group, summed(h, *place(target), side),
                     lambda: landing(way, kind), to[way])

            for way in (0, 1):
                event(s, h, (tag, "s", way), [], needs[way], lambda way=way: go(way, 1))
                event(s, h, (tag, "d", way), [], needs[1 - way], lambda way=way: go(way, 0))

                def onward(way=way):
                    here = summed(h, *place(GOES[way]), sides[way])()
                    total = here[...].astype(jnp.float32) + landing(way, 1)[...].astype(jnp.float32)
                    here[...] = total.astype(jnp.bfloat16)
                    go(way, 2)

                event(s, h, (tag, "p", way), [key(tag, way, 1)], [(tag, "s", way)] + needs[way], onward)

                def finish(way=way):
                    here = summed(h, *place(OWN), sides[way])()
                    total = (
                        here[...].astype(jnp.float32)
                        + landing(1 - way, 0)[...].astype(jnp.float32)
                        + landing(way, 2)[...].astype(jnp.float32)
                    )
                    here[...] = total.astype(jnp.bfloat16)

                event(s, h, (tag, "t", way), [key(tag, 1 - way, 0), key(tag, way, 2)],
                      [(tag, "d", 1 - way), (tag, "p", way)], finish)
            return [[(tag, "t", 0)], [(tag, "t", 1)]]

        def half_cols(color):
            start, size = COLS[color]
            return pl.ds(start // 2, size // 2)

        finals, arrivals = [], []
        for color in "AB":
            to_mid, to_last = (to_x, to_z) if color == "A" else (to_z, to_x)
            cols = span(color)[0]
            tile = [("tile", color, 0)]
            for y in (1, 0):
                mid = (lambda p, y=y: (OWN, y, p)) if color == "A" else (lambda p, y=y: (p, y, OWN))
                last = (lambda p, y=y: (p, y, ALL)) if color == "A" else (lambda p, y=y: (ALL, y, p))
                ends = ring(
                    f"{color}L{y}", color, to_last, last,
                    lambda way, kind, y=y, color=color: land_last.at[h, y, way, kind, :, :, half_cols(color)],
                    [tile, tile],
                )
                ends = ring(
                    f"{color}M{y}", color, to_mid, mid,
                    lambda way, kind, y=y, color=color: land_mid.at[h, y, way, kind, :, half_cols(color)],
                    ends,
                )
                if y == 1:
                    event(s, h, (color + "Y", "n", 0), [], ends[0] + ends[1], lambda color=color, cols=cols: send(
                        key(color + "Y"), group, summed(h, OWN, 1, OWN, cols),
                        lambda: land_y.at[h, 0, 0, :, cols], partner))
                    finals.append((color + "Y", "n", 0))
                    arrivals.append(key(color + "Y"))
                else:
                    finals += ends[0] + ends[1]
        c_cols = span("C")[0]
        for z in range(4):
            event(s, h, (f"CY{z}", "n", 0), [], [("tile", "C", 0)], lambda z=z: send(
                key("CY", z), group, summed(h, z, 1, ALL, c_cols),
                lambda: land_y.at[h, z, :, :, c_cols], partner))

            def add(z=z):
                here = part.at[h, z, 0, :, :, c_cols]
                total = here[...].astype(jnp.float32) + land_y[h, z, :, :, c_cols].astype(jnp.float32)
                here[...] = total.astype(jnp.bfloat16)

            event(s, h, (f"CY{z}", "a", 0), [key("CY", z)], [(f"CY{z}", "n", 0)], add)
        all_z = [(f"CY{z}", "a", 0) for z in range(4)]
        ends = ring("CZ", "C", to_z, lambda p: (p, 0, ALL),
                    lambda way, kind: land_last.at[h, 0, way, kind, :, :, half_cols("C")], [all_z, all_z])
        for way in (0, 1):
            near = (f"CY{GOES[way]}", "a", 0)
            events[s, h, ("CZ", "s", way)].needs[:] = [(f"CY{FAR}", "a", 0)]
            events[s, h, ("CZ", "d", way)].needs[:] = [near]
            events[s, h, ("CZ", "p", way)].needs[:] = [("CZ", "s", way), near]
            events[s, h, ("CZ", "t", way)].needs.append((f"CY{OWN}", "a", 0))
        ends = ring("CX", "C", to_x, lambda p: (OWN, 0, p),
                    lambda way, kind: land_mid.at[h, 0, way, kind, :, half_cols("C")], ends)
        finals += ends[0] + ends[1]

        def total_of():
            here = pl.ds(h * BLOCK, BLOCK)
            total = source(s, h) + part[h, 0, 0, 0, :, :].astype(jnp.float32)
            ab = pl.ds(0, COLS["C"][0])
            mine[s, here, ab] = (
                total[:, : COLS["C"][0]] + land_y[h, 0, 0, :, ab].astype(jnp.float32)
            ).astype(jnp.bfloat16)
            mine[s, here, c_cols] = total[:, COLS["C"][0] :].astype(jnp.bfloat16)
            send((s, h, "r", "relay", 0), "relay", lambda: mine.at[s, here, :],
                 lambda: relay.at[s, here, :], following)

        event(s, h, ("sum", "e", 0), arrivals, finals, total_of)

    lanes = lax.broadcasted_iota(jnp.int32, (512, EXTRA), 1)

    def hidden_tile(h, j):
        both = jnp.dot(
            rows[h, :, :, :, :, pl.ds(0, width)].reshape(512, width), wide[j],
            preferred_element_type=jnp.float32,
        )
        gate = both[:, :LANE]
        value = gate / (1.0 + jnp.exp(-gate)) * both[:, LANE:]
        hidden[:, pl.ds(pl.multiple_of(j * LANE, LANE), LANE)] = value.astype(jnp.bfloat16)

    def start_part(s, h):
        tags = rows[h, :, :, :, :, pl.ds(width, EXTRA)].reshape(512, EXTRA).astype(jnp.float32)
        share[...] = jnp.sum(jnp.where(lanes == cx, tags, 0.0), 1, keepdims=True)
        drain(("g", s, h))
        drain(("r", s - 1, h))

    def part_tile(h, j):
        cols = pl.ds(pl.multiple_of(j * TILE, TILE), TILE)
        value = jnp.dot(hidden[...], down[:, cols], preferred_element_type=jnp.float32)
        value = (value * share[...]).astype(jnp.bfloat16)
        part[h, :, :, :, :, cols] = value.reshape(4, 2, 4, BLOCK, TILE)

    def finish_all():
        for s in range(STEPS):
            if s == STEPS - 1:
                for h in (0, 1):
                    arrive((s, h, "r", "relay", 0))
            out_ref[s] = relay[s]
        for group in list(flying):
            drain(group)

    for s in range(STEPS):
        for h in (0, 1):
            gather(s, h)
            reduce(s, h)

    replay(
        events, pl.semaphore_wait, barrier, loads, hidden_tile, start_part, part_tile, finish_all,
        tiles, width // TILE,
    )


class Event:
    def __init__(self, keys, needs, run):
        self.keys, self.needs, self.run = keys, list(needs), run


def replay(events, wait, barrier, loads, hidden_tile, start_part, part_tile, finish_all, tiles, ticks):
    names = list(events)
    slots = iter(SCHEDULE)

    def now():
        for n in next(slots):
            events[names[n]].run()

    wait(barrier, 7)
    now()
    for copy in loads:
        copy.wait()
    for s in range(STEPS):
        for h in (0, 1):
            table = [next(slots) for _ in range(tiles + ticks)]

            def during(j, entries):
                for tick, numbers in enumerate(entries):
                    if numbers:
                        @pl.when(j == tick)
                        def _(numbers=numbers):
                            for n in numbers:
                                events[names[n]].run()

            @pl.loop(0, tiles)
            def _(j):
                hidden_tile(h, j)
                during(j, table[:tiles])

            start_part(s, h)

            @pl.loop(0, ticks)
            def _(j):
                part_tile(h, j)
                during(j, table[tiles:])

    finish_all()


def both_steps(pending, arriving, chosen, gain, router, gate_cols, up_cols, down_rows):
    tokens, width = pending.shape
    ff = gate_cols.shape[1]
    bf16 = jnp.bfloat16
    copies = 2 * (2 * 17 + 12 + 2 * 25 + 16 + 2)
    return pl.pallas_call(
        kernel,
        out_shape=jax.ShapeDtypeStruct((STEPS, tokens, width), bf16),
        in_specs=[pl.BlockSpec(memory_space=pltpu.VMEM)] * 5
        + [pl.BlockSpec(memory_space=pl.ANY)] * 3,
        out_specs=pl.BlockSpec(memory_space=pltpu.VMEM),
        scratch_shapes=[
            pltpu.VMEM((2, 4, 2, 4, BLOCK, width + EXTRA), bf16),
            pltpu.VMEM((2, 4, 2, 4, BLOCK, width), bf16),
            pltpu.VMEM((ff // LANE, width, 2 * LANE), bf16),
            pltpu.VMEM((ff, width), bf16),
            pltpu.VMEM((512, ff), bf16),
            pltpu.VMEM((512, 1), jnp.float32),
            pltpu.VMEM((STEPS, tokens, width), bf16),
            pltpu.VMEM((STEPS, tokens, width), bf16),
            pltpu.VMEM((2, 2, 2, 3, 4, BLOCK, width // 2), bf16),
            pltpu.VMEM((2, 2, 2, 3, BLOCK, width // 2), bf16),
            pltpu.VMEM((2, 4, 4, BLOCK, width), bf16),
            pltpu.SemaphoreType.DMA((copies,)),
            pltpu.SemaphoreType.DMA((copies,)),
            pltpu.SemaphoreType.DMA((2 * (ff // LANE) + 1,)),
        ],
        compiler_params=pltpu.CompilerParams(
            collective_id=0, has_side_effects=True, vmem_limit_bytes=66_000_000
        ),
        name="both_steps",
    )(pending, arriving, chosen, gain, router, gate_cols, up_cols, down_rows)


def shards(
    pending_inputs,
    arriving_microgroups,
    expert_assignment,
    segment_rescale_factor,
    assignment_logit_maps,
    gating_projections,
    expanding_projections,
    contracting_projections,
):
    carried = both_steps(
        pending_inputs[0],
        arriving_microgroups[0],
        expert_assignment[0],
        segment_rescale_factor,
        assignment_logit_maps[0].T,
        gating_projections[0],
        expanding_projections[0],
        contracting_projections[0],
    )
    return carried[:, None]


def solution(mesh):
    return jax.shard_map(
        shards,
        mesh=mesh,
        in_specs=(
            P("section", "expert", None),
            P(None, "expert", None),
            P("section", None, "expert", None),
            P("section", None),
            P("section", None, None),
            P("section", None, "expert"),
            P("section", None, "expert"),
            P("section", "expert", None),
        ),
        out_specs=P(None, "section", "expert", None),
        check_vma=False,
    )
```

```python
import jax
import jax.numpy as jnp
from jax import lax
from jax.experimental import pallas as pl
from jax.experimental.pallas import tpu as pltpu
from jax.sharding import PartitionSpec as P

EXPERTS = 4
STEPS = 2
EXTRA = 128
BLOCK = 16
LANE = 128
MESH = pl.DeviceIdType.MESH

epsilon = 1e-05

OWN, PLUS, MINUS, FAR = 0, 1, 2, 3
CAME = (MINUS, PLUS)
GOES = (PLUS, MINUS)
ALL = slice(None)

COLS = {"A": (1024, 1024), "B": (2048, 2048), "C": (0, 1024)}
TAGGED = "C"
TILE = 512

GATHER_PIECES = (("o", OWN), ("n", slice(PLUS, FAR)), ("f", FAR))
REDUCE_PIECES = (("n", slice(OWN, FAR)), ("f", FAR))

SCHEDULE = (
    (0, 85, 87, 90, 92, 1, 8, 10, 43, 45, 47, 50, 52, 241, 326, 328, 242, 3, 5, 284, 331, 333, 291, 293,
     249, 251, 86, 88, 91, 93, 95, 97, 9, 11, 244, 246, 2, 23, 25, 28, 30, 51, 53, 46, 48, 55, 57, 44, 65,
     67, 70, 72, 4, 6, 13, 15, 243, 94, 89, 100, 102, 105, 285, 96, 98, 12, 24, 26, 33, 35, 29, 31, 54, 49,
     60, 62, 66, 68, 75, 77, 56, 58, 14, 16, 101, 106, 71, 103, 107, 73, 7, 18, 20, 27, 38, 40, 99, 34, 61,
     63, 36, 32, 332, 250, 334, 69, 80, 82, 286, 252, 288, 17, 104, 108, 19, 76, 78, 306, 21, 39, 308, 41,
     59, 37, 269, 327, 335, 74, 329, 245, 253, 338, 247, 336, 264, 64, 266, 311, 313, 256, 81, 22, 83, 254,
     289, 292, 79, 287, 298, 42, 330, 346, 343, 296, 341, 248, 261, 259, 339, 337, 309, 267, 270, 314, 307,
     265, 257, 84, 109,),
    (344, 342, 347, 255, 274, 276, 290, 301, 303,),
    (340, 260, 262, 299, 312, 316, 271,),
    (348, 268, 279, 281, 310, 318,),
    (345, 258, 297,),
    (349, 263, 272, 275, 277, 302, 304, 315, 323,),
    (280, 282, 321, 294,),
    (273, 317, 319,),
    (278, 300, 305,),
    (283, 324, 208,),
    (295, 322, 210,),
    (110, 114, 320, 118, 122, 111, 115, 119, 123,),
    (136, 140, 143, 147,),
    (212, 325, 350, 144, 148,),
    (112, 116,),
    (120, 214, 124, 159, 160, 163, 164, 167, 171, 209, 135, 139,),
    (),
    (145, 149, 211, 217, 225, 168, 172,),
    (113, 117, 126, 130, 161, 165,),
    (213, 221, 229, 121, 125, 169, 173, 137, 141,),
    (127, 131, 146, 150, 152, 156, 184, 188,),
    (215, 216, 220, 224, 228, 128, 132, 138, 151, 162, 166, 175, 179, 185, 189, 192, 196,),
    (142,),
    (155, 170, 180, 218, 222, 174, 176, 193, 197,),
    (226, 230, 129, 133, 449,),
    (153, 177, 181, 186, 190, 451,),
    (351, 355, 219, 223, 232, 236, 359, 363, 352, 198, 356, 360, 364,),
    (227, 231, 233, 237, 194, 453, 377, 381, 384, 388,),
    (157, 178, 182, 385, 389,),
    (238, 154, 187, 191, 200, 204, 353, 234, 357,),
    (183, 361, 365, 400, 401, 404, 405, 408, 412, 376, 380, 450, 455, 199, 201, 195, 158, 205, 386, 390,
     409, 413, 239, 235, 452, 458, 466, 134, 206, 354, 358, 202, 367, 371, 402, 406, 362, 366, 368, 454,
     462, 470, 372, 378, 382, 425, 429, 426, 430, 410, 414, 387, 391, 207, 369, 373, 203, 393, 397, 456,
     457, 461, 465, 469, 379, 383, 392, 403, 396, 407, 416, 420, 433, 437, 240, 427, 431, 459, 463, 434,
     438, 467, 471, 411, 421, 415, 417, 370, 374, 375, 418, 422, 482, 460, 464, 473, 477, 394, 398, 567,
     569, 572, 574, 483, 490, 492, 525, 527, 529, 532, 534, 468, 472, 428, 432, 441, 445, 474, 478, 435,
     439, 419, 423, 424, 573, 575, 395, 399, 475, 479, 491, 493, 485, 487, 484, 510, 512, 568, 570, 577,
     579, 505, 507, 528, 530, 526, 547, 537, 549, 539, 576, 494, 511, 513, 436, 443, 446, 440, 442, 447,
     476, 480, 552, 554, 578, 580, 571, 582, 584, 587, 531, 542, 544, 548, 550, 486, 488, 495, 497, 514,
     506, 508, 557, 515, 559, 517, 444, 448, 481, 581, 583, 588, 585, 538, 540, 551, 589, 543, 489, 500,
     502, 545, 496, 509, 520, 522, 498, 553, 555, 723, 586, 590, 516, 518, 562, 564, 808, 810, 813, 815,
     731, 733, 768, 770, 773, 775, 726, 728, 724, 766, 501, 503, 541, 499, 521, 523, 546, 558, 560, 556,
     519, 814, 816, 533, 535, 732, 734, 563, 565, 809, 811, 818, 820, 769, 771, 778, 780, 504, 774, 524,
     776, 817, 727, 735, 729, 736, 738, 561, 725, 746, 748, 751, 753, 819, 821, 536, 772, 783, 785, 566,
     591,),
    (812, 823, 825, 828, 737, 739, 767, 788, 790, 793, 795,),
    (752, 754,),
    (822, 777, 730, 741, 743, 779, 781,),
    (824, 826, 829, 830, 740, 747, 749, 756, 758,),
    (755, 784, 786, 789, 791, 798, 800,),
    (827, 831, 742, 744, 794, 796,),
    (750, 757, 759, 761, 763, 782,),
    (787, 792, 803, 805,),
    (745, 690, 692, 694,),
    (799, 760, 801,),
    (592, 596, 762, 764, 797, 696, 600, 604, 593, 597, 601, 605, 618, 622, 625, 626, 629, 630, 617, 621,),
    (804, 806,),
    (),
    (765, 802, 594, 598,),
    (602, 606, 641, 807, 832, 642, 645, 646, 649, 650, 653, 654, 666, 667, 670, 671, 674, 675, 678, 679,),
    (),
    (627, 631, 691,),
    (595, 599, 608, 612, 619, 623, 643, 647,),
    (651, 693, 655, 699, 707, 603, 607, 609, 613,),
    (620, 624, 628, 632, 633, 634, 637, 638,),
    (695, 703, 711, 668, 672,),
    (),
    (697, 698, 702, 706, 710, 676, 680,),
    (931,),
    (),
    (833, 837, 700, 704, 610, 614, 644, 648, 657, 661,),
    (708, 712, 933,),
    (652, 662, 656, 658, 635,),
    (701, 705, 714, 718, 639, 669, 673, 659, 663, 682, 686, 935,),
    (709, 713, 715, 719, 841, 845, 882, 886, 932, 677, 687, 883, 887, 681, 683, 611, 615, 616, 636, 890,
     894, 720, 834, 716, 838, 640, 660, 664, 665, 835, 839, 842, 846, 684, 688, 934, 937, 884, 888, 940,
     847, 948, 891, 895, 836, 840, 863, 843, 870, 936, 859, 944, 717, 721, 892, 896, 685, 689, 952, 866,
     885, 889, 722, 867, 848, 871, 849, 853, 898, 902, 850, 911, 844, 907, 858, 872, 854, 908, 912, 938,
     939, 947, 943, 915, 919, 951, 893, 897, 899, 903, 868, 904, 851, 855, 909, 913, 941, 873, 862, 860,
     945, 875, 920, 900, 916, 949, 953, 852, 856, 921, 869, 857, 905, 917, 942, 864, 910, 914, 923, 927,
     861, 946, 901, 906, 959, 954, 955, 879, 950, 956, 960, 874, 865, 878, 922, 924, 929, 918, 961, 925,
     928, 957, 876, 880, 962, 930, 958, 926, 877, 881, 963,),
)


def kernel(
    pending_ref, arriving_ref, chosen_ref, gain_ref, router_ref, gate_hbm, up_hbm, down_hbm, out_ref,
    rows, part, wide, down, hidden, share, mine, relay,
    land_last, land_mid, land_y,
    send_sems, recv_sems, load_sems,
):
    width = pending_ref.shape[1]
    tiles = down.shape[0] // LANE
    section = lax.axis_index("section")
    e = lax.axis_index("expert")
    cx, cy, cz = e // 8, (e // 4) % 2, e % 4

    def at(x, y, z):
        return {"section": section, "expert": x * 8 + y * 4 + z}

    to_x = (at(lax.rem(cx + 1, 4), cy, cz), at(lax.rem(cx + 3, 4), cy, cz))
    to_z = (at(cx, cy, lax.rem(cz + 1, 4)), at(cx, cy, lax.rem(cz + 3, 4)))
    partner = at(cx, 1 - cy, cz)
    following = {"section": lax.rem(section + 1, 4), "expert": e}
    preceding = {"section": lax.rem(section + 3, 4), "expert": e}

    loads = []

    def load(src, dst):
        copy = pltpu.make_async_copy(src, dst, load_sems.at[len(loads)])
        copy.start()
        loads.append(copy)

    for j in range(tiles):
        load(gate_hbm.at[:, pl.ds(j * LANE, LANE)], wide.at[j, :, pl.ds(0, LANE)])
        load(up_hbm.at[:, pl.ds(j * LANE, LANE)], wide.at[j, :, pl.ds(LANE, LANE)])
    load(down_hbm, down)

    barrier = pltpu.get_barrier_semaphore()
    for device in (*to_x, *to_z, partner, following, preceding):
        pl.semaphore_signal(barrier, inc=1, device_id=device, device_id_type=MESH)

    numbers = {}
    known = {}
    flying = {}

    def send(key, group, src, dst, device):
        n = numbers.setdefault(key if "relay" in key else key[1:], len(numbers))
        known[key] = lambda: pltpu.make_async_remote_copy(
            src_ref=src(), dst_ref=dst(), send_sem=send_sems.at[n], recv_sem=recv_sems.at[n],
            device_id=device, device_id_type=MESH,
        )
        known[key]().start()
        flying.setdefault(group, []).append(known[key])

    def arrive(key):
        known[key]().wait_recv()

    def drain(group):
        for copy in flying.pop(group, []):
            copy().wait_send()

    def gathered(h, z, y, x, cols):
        return lambda: rows.at[h, z, y, x, :, cols]

    def summed(h, z, y, x, cols):
        return lambda: part.at[h, z, y, x, :, cols]

    def span(color, tags=False):
        start, size = COLS[color]
        if tags:
            start, size = (start, size + EXTRA) if color == TAGGED else (start + EXTRA, size)
        cut = size // 2 // LANE * LANE
        return pl.ds(start, size), (pl.ds(start, cut), pl.ds(start + cut, size - cut))

    def source(s, h):
        here = pl.ds(h * BLOCK, BLOCK)
        if s == 0:
            return pending_ref[here, :].astype(jnp.float32)
        return jnp.where(section == 0, arriving_ref[here, :], relay[0, here, :]).astype(jnp.float32)

    def enter(s, h):
        here = pl.ds(h * BLOCK, BLOCK)
        value = source(s, h)
        mean = jnp.mean(value * value, -1, keepdims=True)
        normed = (value * lax.rsqrt(mean + epsilon) * gain_ref[...]).astype(jnp.bfloat16)
        rows[h, 0, 0, 0, :, pl.ds(EXTRA, width)] = normed
        precise = normed.astype(jnp.float32)
        lane = lax.broadcasted_iota(jnp.int32, (BLOCK, EXTRA), 1)
        first_choice = chosen_ref[s, here, 0:1]
        second_choice = chosen_ref[s, here, 1:2]
        gap = jnp.zeros((BLOCK, 1), jnp.float32)
        for expert in range(EXPERTS):
            logit = jnp.sum(precise * router_ref[expert : expert + 1, :], -1, keepdims=True)
            gap = gap + jnp.where(first_choice == expert, logit, 0.0)
            gap = gap - jnp.where(second_choice == expert, logit, 0.0)
        first = 1.0 / (1.0 + jnp.exp(-gap))
        second = 1.0 - first
        tags = jnp.where(lane == first_choice, first, 0.0) + jnp.where(
            lane == second_choice, second, 0.0
        )
        rows[h, 0, 0, 0, :, pl.ds(0, EXTRA)] = tags.astype(jnp.bfloat16)

    events = {}

    def event(s, h, label, keys, needs, act):
        def run():
            for key in keys:
                arrive(key)
            act()

        events[s, h, label] = Event(keys, needs, run)

    def gather(s, h):
        group = ("g", s, h)

        def key(tag, way=0):
            return (s, h, "g", tag, way)

        def near(tag, color, to, place, way):
            cols = span(color, True)[0]
            send(key(tag, way), group, gathered(h, *place(OWN), cols),
                 gathered(h, *place(CAME[way]), cols), to[way])

        def ring(tag, color, to, place, needs):
            sides = span(color, True)[1]
            for way in (0, 1):
                event(s, h, (tag, "n", way), [], needs,
                      lambda way=way: near(tag, color, to, place, way))

                def forward(way=way):
                    send(key(tag + "f", way), group, gathered(h, *place(CAME[way]), sides[way]),
                         gathered(h, *place(FAR), sides[way]), to[way])

                event(s, h, (tag, "f", way), [key(tag, way)], [(tag, "n", way)], forward)
            event(s, h, (tag, "e", 0), [key(tag + "f", 0), key(tag + "f", 1)],
                  [(tag, "f", 0), (tag, "f", 1)], lambda: None)
            return (tag, "e", 0)

        def across(tag, color, z, x, needs):
            cols = span(color, True)[0]
            event(s, h, (tag, "n", 0), [], needs, lambda: send(
                key(tag), group, gathered(h, z, 0, x, cols), gathered(h, z, 1, x, cols), partner))
            return key(tag)

        ready = ("enter", "e", 0)
        before = [(s - 1, h, "r", "relay", 0)] if s else []
        event(s, h, ready, before, [("sum", "e", 0)] if s else [], lambda: enter(s, h))
        finals, ends = [], []
        for color in "AB":
            to_mid, to_last = (to_x, to_z) if color == "A" else (to_z, to_x)
            crossed = across(color + "y", color, OWN, OWN, [ready])
            event(s, h, (color + "y", "e", 0), [crossed], [(color + "y", "n", 0)], lambda: None)
            for y in (0, 1):
                mid = (lambda p, y=y: (OWN, y, p)) if color == "A" else (lambda p, y=y: (p, y, OWN))
                begun = (color + "y", "e", 0) if y else ready
                tag = f"{color}m{y}"
                end = ring(tag, color, to_mid, mid, [begun])
                near_in = [(tag, "f", 0), (tag, "f", 1)]
                for (name, piece), need in zip(GATHER_PIECES, ([begun], near_in, [end],)):
                    last = (
                        (lambda p, y=y, piece=piece: (p, y, piece))
                        if color == "A"
                        else (lambda p, y=y, piece=piece: (piece, y, p))
                    )
                    ends.append(ring(f"{color}l{y}{name}", color, to_last, last, need))
        end_x = ring("Cx", "C", to_x, lambda p: (OWN, 0, p), [ready])
        near_in = [("Cx", "f", 0), ("Cx", "f", 1)]
        ends_z = [
            ring("Cz" + name, "C", to_z, lambda p, piece=piece: (p, 0, piece), need)
            for (name, piece), need in zip(GATHER_PIECES, ([ready], near_in, [end_x],))
        ]
        came = [[("Cz" + name, "f", way) for name, _ in GATHER_PIECES] for way in (0, 1)]
        for place, need in ((OWN, [end_x] + near_in), (MINUS, came[0]), (PLUS, came[1]), (FAR, ends_z)):
            finals.append(across(f"Cy{place}", "C", place, ALL, need))
        event(s, h, ("gathered", "e", 0), finals, ends + ends_z + [(f"Cy{p}", "n", 0) for p in range(4)],
              lambda: None)

    def reduce(s, h):
        group = ("r", s, h)

        def key(tag, way=0, kind=0):
            return (s, h, "r", tag, way, kind)

        def ring(tag, color, to, place, landing, far, near, own):
            sides = span(color)[1]

            def go(way, kind):
                target = FAR if kind == 1 else GOES[way]
                side = sides[1 - way] if kind == 0 else sides[way]
                send(key(tag, way, kind), group, summed(h, *place(target), side),
                     lambda: landing(way, kind), to[way])

            for way in (0, 1):
                event(s, h, (tag, "s", way), [], far(way), lambda way=way: go(way, 1))
                event(s, h, (tag, "d", way), [], near(way, 1 - way), lambda way=way: go(way, 0))

                def onward(way=way):
                    here = summed(h, *place(GOES[way]), sides[way])()
                    total = here[...].astype(jnp.float32) + landing(way, 1)[...].astype(jnp.float32)
                    here[...] = total.astype(jnp.bfloat16)
                    go(way, 2)

                event(s, h, (tag, "p", way), [key(tag, way, 1)], [(tag, "s", way)] + near(way, way), onward)

                def finish(way=way):
                    here = summed(h, *place(OWN), sides[way])()
                    total = (
                        here[...].astype(jnp.float32)
                        + landing(1 - way, 0)[...].astype(jnp.float32)
                        + landing(way, 2)[...].astype(jnp.float32)
                    )
                    here[...] = total.astype(jnp.bfloat16)

                event(s, h, (tag, "t", way), [key(tag, 1 - way, 0), key(tag, way, 2)],
                      [(tag, "d", 1 - way), (tag, "p", way)] + own(way), finish)
            return [(tag, "t", 0), (tag, "t", 1)]

        def after(tag):
            return (
                lambda side: [(tag + "f", "t", side)],
                lambda way, side: [(tag + "n", "t", side)],
                lambda side: [(tag + "n", "t", side)],
            )

        def half_cols(color):
            start, size = COLS[color]
            return pl.ds(start // 2, size // 2)

        finals, arrivals = [], []
        for color in "AB":
            to_mid, to_last = (to_x, to_z) if color == "A" else (to_z, to_x)
            cols = span(color)[0]
            tile = [("tile", color, 0)]
            for y in (1, 0):
                mid = (lambda p, y=y: (OWN, y, p)) if color == "A" else (lambda p, y=y: (p, y, OWN))
                for name, piece in REDUCE_PIECES[::-1]:
                    last = (
                        (lambda p, y=y, piece=piece: (p, y, piece))
                        if color == "A"
                        else (lambda p, y=y, piece=piece: (piece, y, p))
                    )
                    ring(
                        f"{color}L{y}{name}", color, to_last, last,
                        lambda way, kind, y=y, color=color, piece=piece: land_last.at[
                            h, y, way, kind, piece, :, half_cols(color)
                        ],
                        lambda side: tile, lambda way, side: tile, lambda side: tile,
                    )
                ends = ring(
                    f"{color}M{y}", color, to_mid, mid,
                    lambda way, kind, y=y, color=color: land_mid.at[h, y, way, kind, :, half_cols(color)],
                    *after(f"{color}L{y}"),
                )
                if y == 1:
                    event(s, h, (color + "Y", "n", 0), [], ends, lambda color=color, cols=cols: send(
                        key(color + "Y"), group, summed(h, OWN, 1, OWN, cols),
                        lambda: land_y.at[h, 0, 0, :, cols], partner))
                    finals.append((color + "Y", "n", 0))
                    arrivals.append(key(color + "Y"))
                else:
                    finals += ends
        c_cols = span("C")[0]
        for z in range(4):
            event(s, h, (f"CY{z}", "n", 0), [], [("tile", "C", 0)], lambda z=z: send(
                key("CY", z), group, summed(h, z, 1, ALL, c_cols),
                lambda: land_y.at[h, z, :, :, c_cols], partner))

            def add(z=z):
                here = part.at[h, z, 0, :, :, c_cols]
                total = here[...].astype(jnp.float32) + land_y[h, z, :, :, c_cols].astype(jnp.float32)
                here[...] = total.astype(jnp.bfloat16)

            event(s, h, (f"CY{z}", "a", 0), [key("CY", z)], [(f"CY{z}", "n", 0)], add)
        for name, piece in REDUCE_PIECES[::-1]:
            ring(
                "CZ" + name, "C", to_z, lambda p, piece=piece: (p, 0, piece),
                lambda way, kind, piece=piece: land_last.at[h, 0, way, kind, piece, :, half_cols("C")],
                lambda side: [(f"CY{FAR}", "a", 0)],
                lambda way, side: [(f"CY{GOES[way]}", "a", 0)],
                lambda side: [(f"CY{OWN}", "a", 0)],
            )
        ends = ring("CX", "C", to_x, lambda p: (OWN, 0, p),
                    lambda way, kind: land_mid.at[h, 0, way, kind, :, half_cols("C")], *after("CZ"))
        finals += ends

        def total_of():
            here = pl.ds(h * BLOCK, BLOCK)
            total = source(s, h) + part[h, 0, 0, 0, :, :].astype(jnp.float32)
            for color in "ABC":
                start, size = COLS[color]
                value = total[:, start : start + size]
                if color != "C":
                    value = value + land_y[h, 0, 0, :, start : start + size].astype(jnp.float32)
                mine[s, here, start : start + size] = value.astype(jnp.bfloat16)
            send((s, h, "r", "relay", 0), "relay", lambda: mine.at[s, here, :],
                 lambda: relay.at[s, here, :], following)

        event(s, h, ("sum", "e", 0), arrivals, finals, total_of)

    lanes = lax.broadcasted_iota(jnp.int32, (512, EXTRA), 1)

    def hidden_tile(h, j):
        both = jnp.dot(
            rows[h, :, :, :, :, pl.ds(EXTRA, width)].reshape(512, width), wide[j],
            preferred_element_type=jnp.float32,
        )
        gate = both[:, :LANE]
        value = gate / (1.0 + jnp.exp(-gate)) * both[:, LANE:]
        hidden[:, pl.ds(pl.multiple_of(j * LANE, LANE), LANE)] = value.astype(jnp.bfloat16)

    def start_part(s, h):
        tags = rows[h, :, :, :, :, pl.ds(0, EXTRA)].reshape(512, EXTRA).astype(jnp.float32)
        share[...] = jnp.sum(jnp.where(lanes == cx, tags, 0.0), 1, keepdims=True)
        drain(("g", s, h))
        drain(("r", s - 1, h))

    def part_tile(h, j):
        cols = pl.ds(pl.multiple_of(j * TILE, TILE), TILE)
        value = jnp.dot(hidden[...], down[:, cols], preferred_element_type=jnp.float32)
        value = (value * share[...]).astype(jnp.bfloat16)
        part[h, :, :, :, :, cols] = value.reshape(4, 2, 4, BLOCK, TILE)

    def finish_all():
        for s in range(STEPS):
            if s == STEPS - 1:
                for h in (0, 1):
                    arrive((s, h, "r", "relay", 0))
            out_ref[s] = relay[s]
        for group in list(flying):
            drain(group)

    for s in range(STEPS):
        for h in (0, 1):
            gather(s, h)
            reduce(s, h)

    replay(
        events, pl.semaphore_wait, barrier, loads, hidden_tile, start_part, part_tile, finish_all,
        tiles, width // TILE,
    )


class Event:
    def __init__(self, keys, needs, run):
        self.keys, self.needs, self.run = keys, list(needs), run


def replay(events, wait, barrier, loads, hidden_tile, start_part, part_tile, finish_all, tiles, ticks):
    names = list(events)
    slots = iter(SCHEDULE)

    first, *others = next(slots)
    events[names[first]].run()
    wait(barrier, 7)
    for n in others:
        events[names[n]].run()
    for copy in loads:
        copy.wait()
    for s in range(STEPS):
        for h in (0, 1):
            table = [next(slots) for _ in range(tiles + ticks)]

            def during(j, entries):
                for tick, numbers in enumerate(entries):
                    if numbers:
                        @pl.when(j == tick)
                        def _(numbers=numbers):
                            for n in numbers:
                                events[names[n]].run()

            @pl.loop(0, tiles)
            def _(j):
                hidden_tile(h, j)
                during(j, table[:tiles])

            start_part(s, h)

            @pl.loop(0, ticks)
            def _(j):
                part_tile(h, j)
                during(j, table[tiles:])

    finish_all()


def both_steps(pending, arriving, chosen, gain, router, gate_cols, up_cols, down_rows):
    tokens, width = pending.shape
    ff = gate_cols.shape[1]
    bf16 = jnp.bfloat16
    copies = 368
    return pl.pallas_call(
        kernel,
        out_shape=jax.ShapeDtypeStruct((STEPS, tokens, width), bf16),
        in_specs=[pl.BlockSpec(memory_space=pltpu.VMEM)] * 5
        + [pl.BlockSpec(memory_space=pl.ANY)] * 3,
        out_specs=pl.BlockSpec(memory_space=pltpu.VMEM),
        scratch_shapes=[
            pltpu.VMEM((2, 4, 2, 4, BLOCK, width + EXTRA), bf16),
            pltpu.VMEM((2, 4, 2, 4, BLOCK, width), bf16),
            pltpu.VMEM((ff // LANE, width, 2 * LANE), bf16),
            pltpu.VMEM((ff, width), bf16),
            pltpu.VMEM((512, ff), bf16),
            pltpu.VMEM((512, 1), jnp.float32),
            pltpu.VMEM((STEPS, tokens, width), bf16),
            pltpu.VMEM((STEPS, tokens, width), bf16),
            pltpu.VMEM((2, 2, 2, 3, 4, BLOCK, width // 2), bf16),
            pltpu.VMEM((2, 2, 2, 3, BLOCK, width // 2), bf16),
            pltpu.VMEM((2, 4, 4, BLOCK, width), bf16),
            pltpu.SemaphoreType.DMA((copies,)),
            pltpu.SemaphoreType.DMA((copies,)),
            pltpu.SemaphoreType.DMA((2 * (ff // LANE) + 1,)),
        ],
        compiler_params=pltpu.CompilerParams(
            collective_id=0, has_side_effects=True, vmem_limit_bytes=66_000_000
        ),
        name="both_steps",
    )(pending, arriving, chosen, gain, router, gate_cols, up_cols, down_rows)


def shards(
    pending_inputs,
    arriving_microgroups,
    expert_assignment,
    segment_rescale_factor,
    assignment_logit_maps,
    gating_projections,
    expanding_projections,
    contracting_projections,
):
    carried = both_steps(
        pending_inputs[0],
        arriving_microgroups[0],
        expert_assignment[0],
        segment_rescale_factor,
        assignment_logit_maps[0].T,
        gating_projections[0],
        expanding_projections[0],
        contracting_projections[0],
    )
    return carried[:, None]


def solution(mesh):
    return jax.shard_map(
        shards,
        mesh=mesh,
        in_specs=(
            P("section", "expert", None),
            P(None, "expert", None),
            P("section", None, "expert", None),
            P("section", None),
            P("section", None, None),
            P("section", None, "expert"),
            P("section", None, "expert"),
            P("section", "expert", None),
        ),
        out_specs=P(None, "section", "expert", None),
        check_vma=False,
    )
```

```python
import jax
import jax.numpy as jnp
from jax import lax
from jax.experimental import pallas as pl
from jax.experimental.pallas import tpu as pltpu
from jax.sharding import PartitionSpec as P

EXPERTS = 4
STEPS = 2
EXTRA = 128
BLOCK = 16
LANE = 128
LOGICAL = pl.DeviceIdType.LOGICAL

epsilon = 1e-05

OWN, PLUS, MINUS, FAR = 0, 1, 2, 3
CAME = (MINUS, PLUS)
GOES = (PLUS, MINUS)
ALL = slice(None)

COLS = {"A": (1024, 1024), "B": (2048, 2048), "C": (0, 1024)}
TAGGED = "C"
TILE = 512

GATHER_PIECES = (("o", OWN), ("n", slice(PLUS, FAR)), ("f", FAR))
REDUCE_PIECES = (("n", slice(OWN, FAR)), ("f", FAR))

SCHEDULE = (
    (0, 85, 87, 90, 92, 1, 8, 10, 43, 45, 47, 50, 52, 241, 326, 328, 242, 3, 5, 284, 331, 333, 291, 293,
     249, 251, 86, 88, 91, 93, 95, 97, 9, 11, 244, 246, 2, 23, 25, 28, 30, 51, 53, 46, 48, 55, 57, 44, 65,
     67, 70, 72, 4, 6, 13, 15, 243, 94, 89, 100, 102, 105, 285, 96, 98, 12, 24, 26, 33, 35, 29, 31, 54, 49,
     60, 62, 66, 68, 75, 77, 56, 58, 14, 16, 101, 106, 71, 103, 107, 73, 7, 18, 20, 27, 38, 40, 99, 34, 61,
     63, 36, 32, 332, 250, 334, 69, 80, 82, 286, 252, 288, 17, 104, 108, 19, 76, 78, 306, 21, 39, 308, 41,
     59, 37, 269, 327, 335, 74, 329, 245, 253, 338, 247, 336, 264, 64, 266, 311, 313, 256, 81, 22, 83, 254,
     289, 292, 79, 287, 298, 42, 330, 346, 343, 296, 341, 248, 261, 259, 339, 337, 309, 267, 270, 314, 307,
     265, 257, 84, 109,),
    (344, 342, 347, 255, 274, 276, 290, 301, 303,),
    (340, 260, 262, 299, 312, 316, 271,),
    (348, 268, 279, 281, 310, 318,),
    (345, 258, 297,),
    (349, 263, 272, 275, 277, 302, 304, 315, 323,),
    (280, 282, 321, 294,),
    (273, 317, 319,),
    (278, 300, 305,),
    (283, 324, 208,),
    (295, 322, 210,),
    (110, 114, 320, 118, 122, 111, 115, 119, 123,),
    (136, 140, 143, 147,),
    (212, 325, 350, 144, 148,),
    (112, 116,),
    (120, 214, 124, 159, 160, 163, 164, 167, 171, 209, 135, 139,),
    (),
    (145, 149, 211, 217, 225, 168, 172,),
    (113, 117, 126, 130, 161, 165,),
    (213, 221, 229, 121, 125, 169, 173, 137, 141,),
    (127, 131, 146, 150, 152, 156, 184, 188,),
    (215, 216, 220, 224, 228, 128, 132, 138, 151, 162, 166, 175, 179, 185, 189, 192, 196,),
    (142,),
    (155, 170, 180, 218, 222, 174, 176, 193, 197,),
    (226, 230, 129, 133, 449,),
    (153, 177, 181, 186, 190, 451,),
    (351, 355, 219, 223, 232, 236, 359, 363, 352, 198, 356, 360, 364,),
    (227, 231, 233, 237, 194, 453, 377, 381, 384, 388,),
    (157, 178, 182, 385, 389,),
    (238, 154, 187, 191, 200, 204, 353, 234, 357,),
    (183, 361, 365, 400, 401, 404, 405, 408, 412, 376, 380, 450, 455, 199, 201, 195, 158, 205, 386, 390,
     409, 413, 239, 235, 452, 458, 466, 134, 206, 354, 358, 202, 367, 371, 402, 406, 362, 366, 368, 454,
     462, 470, 372, 378, 382, 425, 429, 426, 430, 410, 414, 387, 391, 207, 369, 373, 203, 393, 397, 456,
     457, 461, 465, 469, 379, 383, 392, 403, 396, 407, 416, 420, 433, 437, 240, 427, 431, 459, 463, 434,
     438, 467, 471, 411, 421, 415, 417, 370, 374, 375, 418, 422, 482, 460, 464, 473, 477, 394, 398, 567,
     569, 572, 574, 483, 490, 492, 525, 527, 529, 532, 534, 468, 472, 428, 432, 441, 445, 474, 478, 435,
     439, 419, 423, 424, 573, 575, 395, 399, 475, 479, 491, 493, 485, 487, 484, 510, 512, 568, 570, 577,
     579, 505, 507, 528, 530, 526, 547, 537, 549, 539, 576, 494, 511, 513, 436, 443, 446, 440, 442, 447,
     476, 480, 552, 554, 578, 580, 571, 582, 584, 587, 531, 542, 544, 548, 550, 486, 488, 495, 497, 514,
     506, 508, 557, 515, 559, 517, 444, 448, 481, 581, 583, 588, 585, 538, 540, 551, 589, 543, 489, 500,
     502, 545, 496, 509, 520, 522, 498, 553, 555, 723, 586, 590, 516, 518, 562, 564, 808, 810, 813, 815,
     731, 733, 768, 770, 773, 775, 726, 728, 724, 766, 501, 503, 541, 499, 521, 523, 546, 558, 560, 556,
     519, 814, 816, 533, 535, 732, 734, 563, 565, 809, 811, 818, 820, 769, 771, 778, 780, 504, 774, 524,
     776, 817, 727, 735, 729, 736, 738, 561, 725, 746, 748, 751, 753, 819, 821, 536, 772, 783, 785, 566,
     591,),
    (812, 823, 825, 828, 737, 739, 767, 788, 790, 793, 795,),
    (752, 754,),
    (822, 777, 730, 741, 743, 779, 781,),
    (824, 826, 829, 830, 740, 747, 749, 756, 758,),
    (755, 784, 786, 789, 791, 798, 800,),
    (827, 831, 742, 744, 794, 796,),
    (750, 757, 759, 761, 763, 782,),
    (787, 792, 803, 805,),
    (745, 690, 692, 694,),
    (799, 760, 801,),
    (592, 596, 762, 764, 797, 696, 600, 604, 593, 597, 601, 605, 618, 622, 625, 626, 629, 630, 617, 621,),
    (804, 806,),
    (),
    (765, 802, 594, 598,),
    (602, 606, 641, 807, 832, 642, 645, 646, 649, 650, 653, 654, 666, 667, 670, 671, 674, 675, 678, 679,),
    (),
    (627, 631, 691,),
    (595, 599, 608, 612, 619, 623, 643, 647,),
    (651, 693, 655, 699, 707, 603, 607, 609, 613,),
    (620, 624, 628, 632, 633, 634, 637, 638,),
    (695, 703, 711, 668, 672,),
    (),
    (697, 698, 702, 706, 710, 676, 680,),
    (931,),
    (),
    (833, 837, 700, 704, 610, 614, 644, 648, 657, 661,),
    (708, 712, 933,),
    (652, 662, 656, 658, 635,),
    (701, 705, 714, 718, 639, 669, 673, 659, 663, 682, 686, 935,),
    (709, 713, 715, 719, 841, 845, 882, 886, 932, 677, 687, 883, 887, 681, 683, 611, 615, 616, 636, 890,
     894, 720, 834, 716, 838, 640, 660, 664, 665, 835, 839, 842, 846, 684, 688, 934, 937, 884, 888, 940,
     847, 948, 891, 895, 836, 840, 863, 843, 870, 936, 859, 944, 717, 721, 892, 896, 685, 689, 952, 866,
     885, 889, 722, 867, 848, 871, 849, 853, 898, 902, 850, 911, 844, 907, 858, 872, 854, 908, 912, 938,
     939, 947, 943, 915, 919, 951, 893, 897, 899, 903, 868, 904, 851, 855, 909, 913, 941, 873, 862, 860,
     945, 875, 920, 900, 916, 949, 953, 852, 856, 921, 869, 857, 905, 917, 942, 864, 910, 914, 923, 927,
     861, 946, 901, 906, 959, 954, 955, 879, 950, 956, 960, 874, 865, 878, 922, 924, 929, 918, 961, 925,
     928, 957, 876, 880, 962, 930, 958, 926, 877, 881, 963,),
)


def kernel(
    pending_ref, arriving_ref, chosen_ref, gain_ref, router_ref, gate_hbm, up_hbm, down_hbm, out_ref,
    rows, part, wide, down, hidden, share, mine, relay,
    land_last, land_mid, land_y,
    send_sems, recv_sems, load_sems,
):
    width = pending_ref.shape[1]
    tiles = down.shape[0] // LANE
    section = lax.axis_index("section")
    e = lax.axis_index("expert")
    cx, cy, cz = e // 8, (e // 4) % 2, e % 4

    def at(x, y, z):
        return section * 32 + x * 8 + y * 4 + z

    to_x = (at(lax.rem(cx + 1, 4), cy, cz), at(lax.rem(cx + 3, 4), cy, cz))
    to_z = (at(cx, cy, lax.rem(cz + 1, 4)), at(cx, cy, lax.rem(cz + 3, 4)))
    partner = at(cx, 1 - cy, cz)
    following = lax.rem(section + 1, 4) * 32 + e
    preceding = lax.rem(section + 3, 4) * 32 + e

    loads = []

    def load(src, dst):
        copy = pltpu.make_async_copy(src, dst, load_sems.at[len(loads)])
        copy.start()
        loads.append(copy)

    for j in range(tiles):
        load(gate_hbm.at[:, pl.ds(j * LANE, LANE)], wide.at[j, :, pl.ds(0, LANE)])
        load(up_hbm.at[:, pl.ds(j * LANE, LANE)], wide.at[j, :, pl.ds(LANE, LANE)])
    load(down_hbm, down)

    barrier = pltpu.get_barrier_semaphore()
    for device in (*to_x, *to_z, partner, following, preceding):
        pl.semaphore_signal(barrier, inc=1, device_id=device, device_id_type=LOGICAL)

    numbers = {}
    known = {}
    flying = {}

    def send(key, group, src, dst, device):
        n = numbers.setdefault(key if "relay" in key else key[1:], len(numbers))
        known[key] = lambda: pltpu.make_async_remote_copy(
            src_ref=src(), dst_ref=dst(), send_sem=send_sems.at[n], recv_sem=recv_sems.at[n],
            device_id=device, device_id_type=LOGICAL,
        )
        known[key]().start()
        flying.setdefault(group, []).append(known[key])

    def arrive(key):
        known[key]().wait_recv()

    def drain(group):
        for copy in flying.pop(group, []):
            copy().wait_send()

    def gathered(h, z, y, x, cols):
        return lambda: rows.at[h, z, y, x, :, cols]

    def summed(h, z, y, x, cols):
        return lambda: part.at[h, z, y, x, :, cols]

    def span(color, tags=False):
        start, size = COLS[color]
        if tags:
            start, size = (start, size + EXTRA) if color == TAGGED else (start + EXTRA, size)
        cut = size // 2 // LANE * LANE
        return pl.ds(start, size), (pl.ds(start, cut), pl.ds(start + cut, size - cut))

    def source(s, h):
        here = pl.ds(h * BLOCK, BLOCK)
        if s == 0:
            return pending_ref[here, :].astype(jnp.float32)
        return jnp.where(section == 0, arriving_ref[here, :], relay[0, here, :]).astype(jnp.float32)

    def enter(s, h):
        here = pl.ds(h * BLOCK, BLOCK)
        value = source(s, h)
        mean = jnp.mean(value * value, -1, keepdims=True)
        normed = (value * lax.rsqrt(mean + epsilon) * gain_ref[...]).astype(jnp.bfloat16)
        rows[h, 0, 0, 0, :, pl.ds(EXTRA, width)] = normed
        precise = normed.astype(jnp.float32)
        lane = lax.broadcasted_iota(jnp.int32, (BLOCK, EXTRA), 1)
        first_choice = chosen_ref[s, here, 0:1]
        second_choice = chosen_ref[s, here, 1:2]
        gap = jnp.zeros((BLOCK, 1), jnp.float32)
        for expert in range(EXPERTS):
            logit = jnp.sum(precise * router_ref[expert : expert + 1, :], -1, keepdims=True)
            gap = gap + jnp.where(first_choice == expert, logit, 0.0)
            gap = gap - jnp.where(second_choice == expert, logit, 0.0)
        first = 1.0 / (1.0 + jnp.exp(-gap))
        second = 1.0 - first
        tags = jnp.where(lane == first_choice, first, 0.0) + jnp.where(
            lane == second_choice, second, 0.0
        )
        rows[h, 0, 0, 0, :, pl.ds(0, EXTRA)] = tags.astype(jnp.bfloat16)

    events = {}

    def event(s, h, label, keys, needs, act):
        def run():
            for key in keys:
                arrive(key)
            act()

        events[s, h, label] = Event(keys, needs, run)

    def gather(s, h):
        group = ("g", s, h)

        def key(tag, way=0):
            return (s, h, "g", tag, way)

        def near(tag, color, to, place, way):
            cols = span(color, True)[0]
            send(key(tag, way), group, gathered(h, *place(OWN), cols),
                 gathered(h, *place(CAME[way]), cols), to[way])

        def ring(tag, color, to, place, needs):
            sides = span(color, True)[1]
            for way in (0, 1):
                event(s, h, (tag, "n", way), [], needs,
                      lambda way=way: near(tag, color, to, place, way))

                def forward(way=way):
                    send(key(tag + "f", way), group, gathered(h, *place(CAME[way]), sides[way]),
                         gathered(h, *place(FAR), sides[way]), to[way])

                event(s, h, (tag, "f", way), [key(tag, way)], [(tag, "n", way)], forward)
            event(s, h, (tag, "e", 0), [key(tag + "f", 0), key(tag + "f", 1)],
                  [(tag, "f", 0), (tag, "f", 1)], lambda: None)
            return (tag, "e", 0)

        def across(tag, color, z, x, needs):
            cols = span(color, True)[0]
            event(s, h, (tag, "n", 0), [], needs, lambda: send(
                key(tag), group, gathered(h, z, 0, x, cols), gathered(h, z, 1, x, cols), partner))
            return key(tag)

        ready = ("enter", "e", 0)
        before = [(s - 1, h, "r", "relay", 0)] if s else []
        event(s, h, ready, before, [("sum", "e", 0)] if s else [], lambda: enter(s, h))
        finals, ends = [], []
        for color in "AB":
            to_mid, to_last = (to_x, to_z) if color == "A" else (to_z, to_x)
            crossed = across(color + "y", color, OWN, OWN, [ready])
            event(s, h, (color + "y", "e", 0), [crossed], [(color + "y", "n", 0)], lambda: None)
            for y in (0, 1):
                mid = (lambda p, y=y: (OWN, y, p)) if color == "A" else (lambda p, y=y: (p, y, OWN))
                begun = (color + "y", "e", 0) if y else ready
                tag = f"{color}m{y}"
                end = ring(tag, color, to_mid, mid, [begun])
                near_in = [(tag, "f", 0), (tag, "f", 1)]
                for (name, piece), need in zip(GATHER_PIECES, ([begun], near_in, [end],)):
                    last = (
                        (lambda p, y=y, piece=piece: (p, y, piece))
                        if color == "A"
                        else (lambda p, y=y, piece=piece: (piece, y, p))
                    )
                    ends.append(ring(f"{color}l{y}{name}", color, to_last, last, need))
        end_x = ring("Cx", "C", to_x, lambda p: (OWN, 0, p), [ready])
        near_in = [("Cx", "f", 0), ("Cx", "f", 1)]
        ends_z = [
            ring("Cz" + name, "C", to_z, lambda p, piece=piece: (p, 0, piece), need)
            for (name, piece), need in zip(GATHER_PIECES, ([ready], near_in, [end_x],))
        ]
        came = [[("Cz" + name, "f", way) for name, _ in GATHER_PIECES] for way in (0, 1)]
        for place, need in ((OWN, [end_x] + near_in), (MINUS, came[0]), (PLUS, came[1]), (FAR, ends_z)):
            finals.append(across(f"Cy{place}", "C", place, ALL, need))
        event(s, h, ("gathered", "e", 0), finals, ends + ends_z + [(f"Cy{p}", "n", 0) for p in range(4)],
              lambda: None)

    def reduce(s, h):
        group = ("r", s, h)

        def key(tag, way=0, kind=0):
            return (s, h, "r", tag, way, kind)

        def ring(tag, color, to, place, landing, far, near, own):
            sides = span(color)[1]

            def go(way, kind):
                target = FAR if kind == 1 else GOES[way]
                side = sides[1 - way] if kind == 0 else sides[way]
                send(key(tag, way, kind), group, summed(h, *place(target), side),
                     lambda: landing(way, kind), to[way])

            for way in (0, 1):
                event(s, h, (tag, "s", way), [], far(way), lambda way=way: go(way, 1))
                event(s, h, (tag, "d", way), [], near(way, 1 - way), lambda way=way: go(way, 0))

                def onward(way=way):
                    here = summed(h, *place(GOES[way]), sides[way])()
                    total = here[...].astype(jnp.float32) + landing(way, 1)[...].astype(jnp.float32)
                    here[...] = total.astype(jnp.bfloat16)
                    go(way, 2)

                event(s, h, (tag, "p", way), [key(tag, way, 1)], [(tag, "s", way)] + near(way, way), onward)

                def finish(way=way):
                    here = summed(h, *place(OWN), sides[way])()
                    total = (
                        here[...].astype(jnp.float32)
                        + landing(1 - way, 0)[...].astype(jnp.float32)
                        + landing(way, 2)[...].astype(jnp.float32)
                    )
                    here[...] = total.astype(jnp.bfloat16)

                event(s, h, (tag, "t", way), [key(tag, 1 - way, 0), key(tag, way, 2)],
                      [(tag, "d", 1 - way), (tag, "p", way)] + own(way), finish)
            return [(tag, "t", 0), (tag, "t", 1)]

        def after(tag):
            return (
                lambda side: [(tag + "f", "t", side)],
                lambda way, side: [(tag + "n", "t", side)],
                lambda side: [(tag + "n", "t", side)],
            )

        def half_cols(color):
            start, size = COLS[color]
            return pl.ds(start // 2, size // 2)

        finals, arrivals = [], []
        for color in "AB":
            to_mid, to_last = (to_x, to_z) if color == "A" else (to_z, to_x)
            cols = span(color)[0]
            tile = [("tile", color, 0)]
            for y in (1, 0):
                mid = (lambda p, y=y: (OWN, y, p)) if color == "A" else (lambda p, y=y: (p, y, OWN))
                for name, piece in REDUCE_PIECES[::-1]:
                    last = (
                        (lambda p, y=y, piece=piece: (p, y, piece))
                        if color == "A"
                        else (lambda p, y=y, piece=piece: (piece, y, p))
                    )
                    ring(
                        f"{color}L{y}{name}", color, to_last, last,
                        lambda way, kind, y=y, color=color, piece=piece: land_last.at[
                            h, y, way, kind, piece, :, half_cols(color)
                        ],
                        lambda side: tile, lambda way, side: tile, lambda side: tile,
                    )
                ends = ring(
                    f"{color}M{y}", color, to_mid, mid,
                    lambda way, kind, y=y, color=color: land_mid.at[h, y, way, kind, :, half_cols(color)],
                    *after(f"{color}L{y}"),
                )
                if y == 1:
                    event(s, h, (color + "Y", "n", 0), [], ends, lambda color=color, cols=cols: send(
                        key(color + "Y"), group, summed(h, OWN, 1, OWN, cols),
                        lambda: land_y.at[h, 0, 0, :, cols], partner))
                    finals.append((color + "Y", "n", 0))
                    arrivals.append(key(color + "Y"))
                else:
                    finals += ends
        c_cols = span("C")[0]
        for z in range(4):
            event(s, h, (f"CY{z}", "n", 0), [], [("tile", "C", 0)], lambda z=z: send(
                key("CY", z), group, summed(h, z, 1, ALL, c_cols),
                lambda: land_y.at[h, z, :, :, c_cols], partner))

            def add(z=z):
                here = part.at[h, z, 0, :, :, c_cols]
                total = here[...].astype(jnp.float32) + land_y[h, z, :, :, c_cols].astype(jnp.float32)
                here[...] = total.astype(jnp.bfloat16)

            event(s, h, (f"CY{z}", "a", 0), [key("CY", z)], [(f"CY{z}", "n", 0)], add)
        for name, piece in REDUCE_PIECES[::-1]:
            ring(
                "CZ" + name, "C", to_z, lambda p, piece=piece: (p, 0, piece),
                lambda way, kind, piece=piece: land_last.at[h, 0, way, kind, piece, :, half_cols("C")],
                lambda side: [(f"CY{FAR}", "a", 0)],
                lambda way, side: [(f"CY{GOES[way]}", "a", 0)],
                lambda side: [(f"CY{OWN}", "a", 0)],
            )
        ends = ring("CX", "C", to_x, lambda p: (OWN, 0, p),
                    lambda way, kind: land_mid.at[h, 0, way, kind, :, half_cols("C")], *after("CZ"))
        finals += ends

        def total_of():
            here = pl.ds(h * BLOCK, BLOCK)
            total = source(s, h) + part[h, 0, 0, 0, :, :].astype(jnp.float32)
            for color in "ABC":
                start, size = COLS[color]
                value = total[:, start : start + size]
                if color != "C":
                    value = value + land_y[h, 0, 0, :, start : start + size].astype(jnp.float32)
                mine[s, here, start : start + size] = value.astype(jnp.bfloat16)
            send((s, h, "r", "relay", 0), "relay", lambda: mine.at[s, here, :],
                 lambda: relay.at[s, here, :], following)

        event(s, h, ("sum", "e", 0), arrivals, finals, total_of)

    lanes = lax.broadcasted_iota(jnp.int32, (512, EXTRA), 1)

    def hidden_tile(h, j):
        both = jnp.dot(
            rows[h, :, :, :, :, pl.ds(EXTRA, width)].reshape(512, width), wide[j],
            preferred_element_type=jnp.float32,
        )
        gate = both[:, :LANE]
        value = gate / (1.0 + jnp.exp(-gate)) * both[:, LANE:]
        hidden[:, pl.ds(pl.multiple_of(j * LANE, LANE), LANE)] = value.astype(jnp.bfloat16)

    def start_part(s, h):
        tags = rows[h, :, :, :, :, pl.ds(0, EXTRA)].reshape(512, EXTRA).astype(jnp.float32)
        share[...] = jnp.sum(jnp.where(lanes == cx, tags, 0.0), 1, keepdims=True)
        drain(("g", s, h))
        drain(("r", s - 1, h))

    def part_tile(h, j):
        cols = pl.ds(pl.multiple_of(j * TILE, TILE), TILE)
        value = jnp.dot(hidden[...], down[:, cols], preferred_element_type=jnp.float32)
        value = (value * share[...]).astype(jnp.bfloat16)
        part[h, :, :, :, :, cols] = value.reshape(4, 2, 4, BLOCK, TILE)

    def finish_all():
        for s in range(STEPS):
            if s == STEPS - 1:
                for h in (0, 1):
                    arrive((s, h, "r", "relay", 0))
            out_ref[s] = relay[s]
        for group in list(flying):
            drain(group)

    for s in range(STEPS):
        for h in (0, 1):
            gather(s, h)
            reduce(s, h)

    replay(
        events, pl.semaphore_wait, barrier, loads, hidden_tile, start_part, part_tile, finish_all,
        tiles, width // TILE,
    )


class Event:
    def __init__(self, keys, needs, run):
        self.keys, self.needs, self.run = keys, list(needs), run


def replay(events, wait, barrier, loads, hidden_tile, start_part, part_tile, finish_all, tiles, ticks):
    names = list(events)
    slots = iter(SCHEDULE)

    first, *others = next(slots)
    events[names[first]].run()
    wait(barrier, 7)
    for n in others:
        events[names[n]].run()
    for copy in loads:
        copy.wait()
    for s in range(STEPS):
        for h in (0, 1):
            table = [next(slots) for _ in range(tiles + ticks)]

            def during(j, entries):
                for tick, numbers in enumerate(entries):
                    if numbers:
                        @pl.when(j == tick)
                        def _(numbers=numbers):
                            for n in numbers:
                                events[names[n]].run()

            @pl.loop(0, tiles)
            def _(j):
                hidden_tile(h, j)
                during(j, table[:tiles])

            start_part(s, h)

            @pl.loop(0, ticks)
            def _(j):
                part_tile(h, j)
                during(j, table[tiles:])

    finish_all()


def both_steps(pending, arriving, chosen, gain, router, gate_cols, up_cols, down_rows):
    tokens, width = pending.shape
    ff = gate_cols.shape[1]
    bf16 = jnp.bfloat16
    copies = 368
    return pl.pallas_call(
        kernel,
        out_shape=jax.ShapeDtypeStruct((STEPS, tokens, width), bf16),
        in_specs=[pl.BlockSpec(memory_space=pltpu.VMEM)] * 5
        + [pl.BlockSpec(memory_space=pl.ANY)] * 3,
        out_specs=pl.BlockSpec(memory_space=pltpu.VMEM),
        scratch_shapes=[
            pltpu.VMEM((2, 4, 2, 4, BLOCK, width + EXTRA), bf16),
            pltpu.VMEM((2, 4, 2, 4, BLOCK, width), bf16),
            pltpu.VMEM((ff // LANE, width, 2 * LANE), bf16),
            pltpu.VMEM((ff, width), bf16),
            pltpu.VMEM((512, ff), bf16),
            pltpu.VMEM((512, 1), jnp.float32),
            pltpu.VMEM((STEPS, tokens, width), bf16),
            pltpu.VMEM((STEPS, tokens, width), bf16),
            pltpu.VMEM((2, 2, 2, 3, 4, BLOCK, width // 2), bf16),
            pltpu.VMEM((2, 2, 2, 3, BLOCK, width // 2), bf16),
            pltpu.VMEM((2, 4, 4, BLOCK, width), bf16),
            pltpu.SemaphoreType.DMA((copies,)),
            pltpu.SemaphoreType.DMA((copies,)),
            pltpu.SemaphoreType.DMA((2 * (ff // LANE) + 1,)),
        ],
        compiler_params=pltpu.CompilerParams(
            collective_id=0, has_side_effects=True, vmem_limit_bytes=66_000_000
        ),
        name="both_steps",
    )(pending, arriving, chosen, gain, router, gate_cols, up_cols, down_rows)


def shards(
    pending_inputs,
    arriving_microgroups,
    expert_assignment,
    segment_rescale_factor,
    assignment_logit_maps,
    gating_projections,
    expanding_projections,
    contracting_projections,
):
    carried = both_steps(
        pending_inputs[0],
        arriving_microgroups[0],
        expert_assignment[0],
        segment_rescale_factor,
        assignment_logit_maps[0].T,
        gating_projections[0],
        expanding_projections[0],
        contracting_projections[0],
    )
    return carried[:, None]


def solution(mesh):
    return jax.shard_map(
        shards,
        mesh=mesh,
        in_specs=(
            P("section", "expert", None),
            P(None, "expert", None),
            P("section", None, "expert", None),
            P("section", None),
            P("section", None, None),
            P("section", None, "expert"),
            P("section", None, "expert"),
            P("section", "expert", None),
        ),
        out_specs=P(None, "section", "expert", None),
        check_vma=False,
    )
```
